32 devices in a mesh: groups: 2 (over y), ctx: 8 (over z, x), col: 2 (over core).
Axes of the slice: x: 2, y: 2, z: 4, core: 2. Of those that a mesh axis runs over, the one named last changes fastest.
Arguments:
- activations: bfloat16 [2048, 4096], P(('groups', 'ctx'), 'col'), parts along dimension 0, may hold values from -6 to 6
- gradients: bfloat16 [2048, 14336], P(('groups', 'ctx'), 'col'), parts along dimension 0, may hold values from -6 to 6
- doc_ids: int32 [2048], P(('groups', 'ctx')), parts along dimension 0, may hold values from 0 to 11, as said below
- proj_in: bfloat16 [4096, 64], P('col'), may hold values from -0.046875 to 0.046875
- proj_out: bfloat16 [14336, 64], P('col'), may hold values from -0.0234375 to 0.0234375
- inverse: float32 [4096, 4096], P('col', 'ctx')
- store_rows: bfloat16 [2048, 4096], P(('groups', 'ctx', 'col')), parts along dimension 0, may hold values from -0.09375 to 0.09375
Outputs:
- scores: float32 [12, 2048], P(None, ('groups', 'ctx', 'col')), parts along dimension 1
The draws below stay inside these ranges and needn't reach their ends.
There are 2 independent parts, one for each index of `groups`. The reference program is written for one: setup_inputs(seed, part) draws one part's arguments, and reference() takes and returns one part's arrays. A program takes and returns all parts, laid end to end along the dimension named above; an argument that names none is the same for every part. Nothing has to cross between parts.
Inputs may be any that keep to these rules, and one draw needn't show every extreme that they name: `doc_ids`: document numbers never fall and rise by at most one from a token to the next, starting at 0. Every aligned block of 128 tokens holds the last token of one or two documents; the last token of the sequence ends document 12 - 1.
All inputs are finite; a program needn't handle non-finite values.
Results may differ from the reference program's by a relative error of at most 0.0029.
Values may be sent and summed in bfloat16 or wider, within the bound.
A program may use at most 64 MiB of HBM per device.

```python
import jax
import jax.numpy as jnp
from jax import lax

D = 4096
FF = 14336
R = 64
F = 4096
TOK_DEV = 128
TOKENS = 1024
NDOC = 12
STORE = 1024


def draw_doc_ids(key, part):
    block_count = TOKENS // TOK_DEV
    key_perm = jax.random.fold_in(key, 11)
    key_late = jax.random.fold_in(key, 12)
    key_early = jax.random.fold_in(key, 13)
    ranking = jax.random.permutation(key_perm, block_count)
    has_two = ranking < block_count // 2
    late_end = jax.random.randint(key_late, (block_count,), TOK_DEV // 2, TOK_DEV)
    late_end = jnp.where(jnp.arange(block_count) == block_count - 1, TOK_DEV - 1, late_end)
    early_end = jax.random.randint(key_early, (block_count,), 0, TOK_DEV // 2)
    position = jnp.arange(TOK_DEV)[None, :]
    is_end = (position == late_end[:, None]) | has_two[:, None] & (position == early_end[:, None])
    flat_end = is_end.reshape(TOKENS).astype(jnp.int32)
    return (jnp.cumsum(flat_end) - flat_end).astype(jnp.int32)


def draw_inverse(key, part):
    key_diag = jax.random.fold_in(key, 21)
    key_off = jax.random.fold_in(key, 22)
    diagonal = jnp.exp(jax.random.uniform(key_diag, (F,), jnp.float32, jnp.log(0.5), jnp.log(2.0)))
    offdiag = jax.random.normal(key_off, (F, F), jnp.float32) * (0.5 / jnp.sqrt(jnp.float32(F)))
    matrix = offdiag + jnp.diag(diagonal)
    return matrix.astype(jnp.float32)


def steps_of(rng, dims, cuts, low, largest):
    factor_of = 1.0
    for axis_at, blocks in cuts:
        steps = jax.random.uniform(jax.random.fold_in(jax.random.fold_in(rng, 6), axis_at), (blocks,), jnp.float32, low / len(cuts), largest / len(cuts))
        factor_of = factor_of * jnp.repeat(jnp.exp(steps), dims[axis_at] // blocks).reshape((-1,) + (1,) * (len(dims) - 1 - axis_at))
    return factor_of


def centred(key, shape, deviation, most, cuts=(), kind=jnp.bfloat16):
    level = steps_of(key, shape, cuts, -0.22, 0.18) if cuts else 1.0
    result = jax.random.normal(key, shape, jnp.float32) * deviation * level
    return jnp.minimum(jnp.maximum(result, -most), most).astype(kind)


def setup_inputs(seed: int = 0, part: int = 0) -> dict:
    keys = jax.random.split(jax.random.key(seed), 8)
    part_keys = jax.random.split(jax.random.fold_in(keys[7], part), 8)
    activations = centred(part_keys[0], (TOKENS, D), 1.0, 6.0, ((0, 8), (1, 2)))
    gradients = centred(part_keys[1], (TOKENS, FF), 1.0, 6.0, ((0, 8), (1, 2)))
    doc_ids = draw_doc_ids(jax.random.fold_in(jax.random.fold_in(keys[7], part), 71), part)
    proj_in = centred(keys[3], (D, R), (4 * D) ** -0.5, 0.046875, ((0, 2),))
    proj_out = centred(keys[4], (FF, R), (4 * FF) ** -0.5, 0.0234375, ((0, 2),))
    inverse = draw_inverse(jax.random.fold_in(keys[7], 71), part)
    store_rows = centred(part_keys[6], (STORE, F), F ** -0.5, 0.09375, ((0, 16),))
    return {"activations": activations, "gradients": gradients, "doc_ids": doc_ids, "proj_in": proj_in, "proj_out": proj_out, "inverse": inverse, "store_rows": store_rows}


def reference(activations, gradients, doc_ids, proj_in, proj_out, inverse, store_rows):
    proj_left = jnp.dot(activations, proj_in, preferred_element_type=jnp.float32)
    proj_right = jnp.dot(gradients, proj_out, preferred_element_type=jnp.float32)
    token_count = proj_left.shape[0]
    proj_rank = proj_left.shape[1]
    col_blocks = proj_left.reshape(token_count, proj_rank // 8, 8).transpose(1, 0, 2)

    def per_block(block_left):
        outer_rows = (block_left[:, :, None] * proj_right[:, None, :]).reshape(token_count, 8 * proj_rank)
        return jax.ops.segment_sum(outer_rows, doc_ids, num_segments=NDOC)

    block_sums = lax.map(per_block, col_blocks)
    doc_grads = block_sums.transpose(1, 0, 2).reshape(NDOC, proj_rank * proj_rank)
    precond = jnp.dot(doc_grads, inverse, precision=lax.Precision.HIGHEST, preferred_element_type=jnp.float32).astype(jnp.bfloat16)
    return jnp.dot(precond, store_rows.T, preferred_element_type=jnp.float32)
```

```python
import functools

import jax
import jax.numpy as jnp
from jax import lax
from jax.experimental import pallas as pl
from jax.experimental.pallas import tpu as pltpu
from jax.sharding import PartitionSpec as P


def from_behind(block, axis, distance):
    devices = range(lax.axis_size(axis))
    route = [(i - distance, i) for i in devices if i - distance in devices]
    return lax.ppermute(block, axis, route)


def shards(activations, gradients, doc_ids, proj_in, proj_out, inverse, store_rows):
    left_part = jnp.dot(activations, proj_in, preferred_element_type=jnp.float32)
    right_part = jnp.dot(gradients, proj_out, preferred_element_type=jnp.float32)
    proj_left, proj_right = lax.psum((left_part, right_part), "col")
    proj_rank = proj_right.shape[1]
    half_rank = proj_rank // lax.axis_size("col")
    own_half = lax.dynamic_slice_in_dim(proj_left, lax.axis_index("col") * half_rank, half_rank, 1)
    first_doc = doc_ids[0]
    slot_index = doc_ids - first_doc
    onehot = (slot_index[:, None] == jnp.arange(3, dtype=jnp.int32)[None, :]).astype(jnp.float32)
    weighted = (onehot[:, :, None] * own_half[:, None, :]).reshape(own_half.shape[0], 3 * half_rank)
    local_sums = lax.dot_general(
        weighted,
        proj_right,
        (((0,), (0,)), ((), ())),
        precision=lax.Precision.HIGHEST,
        preferred_element_type=jnp.float32,
    ).reshape(3, half_rank * proj_rank)
    doc_count = 3 * lax.axis_size("ctx") // 2
    last_row = lax.dynamic_index_in_dim(local_sums, slot_index[-1], 0, keepdims=False)
    incoming, incoming_id = from_behind((last_row, doc_ids[-1].astype(jnp.float32)), "ctx", 1)
    matches = (incoming_id == first_doc.astype(jnp.float32)).astype(jnp.float32)
    head_row = local_sums[0] + matches * incoming
    owned_rows = jnp.stack([head_row, local_sums[1]])
    owned_ids = (first_doc + jnp.arange(2, dtype=jnp.int32)).astype(jnp.float32)
    gathered, gathered_ids = (
        lax.all_gather(owned_rows, "ctx", axis=0, tiled=True),
        lax.all_gather(owned_ids, "ctx", axis=0, tiled=True),
    )
    positions = jnp.arange(gathered.shape[0], dtype=jnp.int32)
    wanted = jnp.arange(doc_count, dtype=jnp.int32).astype(jnp.float32)
    found = gathered_ids[None, :] == wanted[:, None]
    chosen = jnp.max(jnp.where(found, positions[None, :], -1), axis=1)
    doc_grads = jnp.take(gathered, chosen, axis=0)
    partial_q = jnp.dot(
        doc_grads, inverse, precision=lax.Precision.HIGHEST, preferred_element_type=jnp.float32
    )
    precond = lax.psum(partial_q, "col").astype(jnp.bfloat16)
    return lax.dot_general(
        lax.all_gather(precond, "ctx", axis=1, tiled=True),
        store_rows,
        (((1,), (1,)), ((), ())),
        preferred_element_type=jnp.float32,
    )


LANES = 128
SLOTS = 3
LEFT_CHUNKS = 1
RIGHT_CHUNKS = 4
PARTS = 1
MESH = pl.DeviceIdType.MESH
NT = (((1,), (1,)), ((), ()))


def halves(value):
    high = value.astype(jnp.bfloat16).astype(jnp.float32)
    return high, value - high


def dot_nt(left, right):
    return lax.dot_general(left, right, NT, preferred_element_type=jnp.float32)


def dot(left, right):
    return jnp.dot(left, right, preferred_element_type=jnp.float32)


def await_bytes(ref, sem):
    pltpu.make_async_copy(ref, ref, sem).wait()


def score_kernel(
    n, cols, docs,
    act, grad, ids, pin, pout, inv, store, out,
    xl, xr, inv_v, store_v, inv_hi, inv_lo, store_t, ids_all,
    part, came, full_l, sums, q_part, q_from, q_all,
    load_sem, send_sem, recv_sem,
):
    me = lax.axis_index("ctx")
    core = lax.axis_index("col")
    other = cols - 1 - core
    tokens = act.shape[0]
    rank = pin.shape[0]
    half = rank // cols
    pack = LANES // rank
    groups = half // pack // PARTS
    piece = SLOTS * groups
    depth = groups * LANES
    width = q_part.shape[1]

    def load(src, dst, sem):
        pltpu.make_async_copy(src, dst, load_sem.at[sem]).start()

    stages = []
    for x, w, v, count in ((act, pin, xl, LEFT_CHUNKS), (grad, pout, xr, RIGHT_CHUNKS)):
        step = x.shape[1] // count
        for i in range(count):
            span = pl.ds(i * step, step)
            load(x.at[:, span], v.at[pl.ds(0, tokens), span], len(stages))
            load(w.at[:, span], v.at[pl.ds(tokens, rank), span], len(stages))
            stages.append(v.at[:, span])
    ids_sem, inv_sem, store_sem = (len(stages) + i for i in range(3))
    load(ids, ids_all.at[me], ids_sem)
    load(inv, inv_v, inv_sem)
    load(store, store_v, store_sem)

    barrier = pltpu.get_barrier_semaphore()
    ctx_peers = {r: {"ctx": jnp.bitwise_xor(me, r)} for r in sends_order(n)}
    peers = [
        {"ctx": jnp.bitwise_xor(me, r), "col": jnp.bitwise_xor(core, d)}
        for r in sends_order(n) + [0]
        for d in range(cols)
        if r or d
    ]
    for peer in peers:
        pl.semaphore_signal(barrier, inc=1, device_id=peer, device_id_type=MESH)

    def send(src, dst, at, peer, to=None):
        pltpu.make_async_remote_copy(
            src_ref=src, dst_ref=dst, send_sem=send_sem.at[at], recv_sem=recv_sem.at[at if to is None else to],
            device_id=peer, device_id_type=MESH,
        ).start()

    totals = []
    for first, count in ((0, LEFT_CHUNKS), (LEFT_CHUNKS, RIGHT_CHUNKS)):
        total = None
        for i in range(first, first + count):
            await_bytes(stages[i], load_sem.at[i])
            v = stages[i]
            term = dot_nt(v[tokens:, :], v[:tokens, :])
            total = term if total is None else total + term
        totals.append(total)
    left, right = totals
    part[:half] = left[:half]
    part[half : half + rank] = right
    part[half + rank :] = left[half:]
    pl.semaphore_wait(barrier, len(peers))
    partner = {"col": other}
    span = pl.ds(pl.multiple_of(other * half, half), half + rank)
    send(part.at[span], came.at[span], 0, partner)
    await_bytes(ids_all.at[me], load_sem.at[ids_sem])
    for peer in ctx_peers.values():
        send(ids, ids_all.at[me], 1, peer)
    own_ids = ids_all[me]
    first = own_ids[:, 0:1]
    masks = [(own_ids == first + s).astype(jnp.float32) for s in range(SLOTS)]
    await_bytes(part.at[pl.ds(0, half + rank)], recv_sem.at[0])
    rows = pl.ds(pl.multiple_of(core * (half + rank), half), half)
    full_l[...] = part[rows, :] + came[rows, :]
    highs, lows = [], []
    for p in range(pack):
        lines = full_l[pl.ds(p, PARTS * groups, stride=pack), :]
        high, low = halves(
            jnp.concatenate(
                [lines[c * groups : (c + 1) * groups] * mask for c in range(PARTS) for mask in masks], axis=0
            )
        )
        highs.append(high)
        lows.append(low)
    weights = jnp.concatenate(highs + highs + lows, axis=1).astype(jnp.bfloat16)
    high, low = halves(part[half : half + rank] + came[half : half + rank])
    zero = jnp.zeros_like(high)

    def diagonal(block, p):
        return [block if q == p else zero for q in range(pack)]

    spread = jnp.concatenate(
        [
            jnp.concatenate(diagonal(high, p) + diagonal(low, p) + diagonal(high, p), axis=1)
            for p in range(pack)
        ],
        axis=0,
    ).astype(jnp.bfloat16)
    product = dot_nt(weights, spread)
    mine = pl.ds(pl.multiple_of(me * piece, 8), piece)
    for c in range(PARTS):
        sums[c, mine, :] = product[c * piece : (c + 1) * piece]
    for c in range(PARTS):
        for peer in ctx_peers.values():
            send(sums.at[c, mine], sums.at[c, mine], 2, peer, 4 + c)

    await_bytes(inv_v, load_sem.at[inv_sem])
    band = LANES

    def split(i, carry):
        rows = pl.ds(pl.multiple_of(i * band, band), band)
        high, low = halves(inv_v[rows, :])
        inv_hi[rows, :] = high.astype(jnp.bfloat16)
        inv_lo[rows, :] = low.astype(jnp.bfloat16)
        return carry

    lax.fori_loop(0, inv_v.shape[0] // band, split, 0)
    await_bytes(store_v, load_sem.at[store_sem])
    store_t[...] = store_v[...].T

    await_bytes(ids_all.at[pl.ds(0, n - 1)], recv_sem.at[1])
    doc_rows = q_part.shape[0]
    column = lax.broadcasted_iota(jnp.int32, (1, SLOTS * n), 1)
    doc_of = jnp.zeros((1, SLOTS * n), jnp.int32)
    for b in range(n):
        inside = (column >= b * SLOTS) & (column < (b + 1) * SLOTS)
        doc_of = jnp.where(inside, ids_all[b][:, 0:1] + (column - b * SLOTS), doc_of)
    pick = (lax.broadcasted_iota(jnp.int32, (doc_rows, SLOTS * n), 0) == doc_of).astype(jnp.float32)

    def take(c):
        await_bytes(sums.at[c, pl.ds(0, (n - 1) * piece)], recv_sem.at[4 + c])
        gathered = jnp.concatenate(
            [sums[c, pl.ds(k, SLOTS * n, stride=groups), :] for k in range(groups)], axis=1
        )
        high, low = halves(gathered)
        return jnp.concatenate([high, low], axis=0).astype(jnp.bfloat16), high.astype(jnp.bfloat16)

    def times(c, side, both, high):
        at = pl.ds(c * depth, depth), pl.ds(pl.multiple_of(side * width, width), width)
        main = dot(both, inv_hi[at])
        return main[: SLOTS * n] + main[SLOTS * n :] + dot(high, inv_lo[at])

    def picked(rows):
        return jnp.dot(pick, rows, precision=lax.Precision.HIGHEST, preferred_element_type=jnp.float32)

    theirs, own = 0.0, 0.0
    for c in range(PARTS):
        taken = take(c)
        theirs = theirs + times(c, other, *taken)
        if c < PARTS - 1:
            own = own + times(c, core, *taken)
    q_part[...] = picked(theirs)
    send(q_part, q_from, 3, partner)
    mine = picked(own + times(PARTS - 1, core, *taken))
    await_bytes(q_part, recv_sem.at[3])
    slot = me * cols + core
    q_all[slot] = (mine + q_from[...]).astype(jnp.bfloat16)
    for peer in peers:
        send(q_all.at[slot], q_all.at[slot], 4, peer, 4 + PARTS)
    await_bytes(q_all.at[pl.ds(0, n * cols - 1)], recv_sem.at[4 + PARTS])
    precond = jnp.concatenate([q_all[i] for i in range(n * cols)], axis=1)
    out[...] = dot(precond, store_t[...])[:docs]
    await_bytes(part.at[pl.ds(0, half + rank)], send_sem.at[0])
    await_bytes(ids_all.at[pl.ds(0, n - 1)], send_sem.at[1])
    await_bytes(sums.at[:, pl.ds(0, (n - 1) * piece)], send_sem.at[2])
    await_bytes(q_part, send_sem.at[3])
    await_bytes(q_all.at[pl.ds(0, n * cols - 1)], send_sem.at[4])


def sends_order(n):
    near = [r for r in range(1, n // 2 + 1)]
    return [s for r in near for s in ((n - r, r) if n - r != r else (r,))]


def fused(n, cols, activations, gradients, doc_ids, proj_in, proj_out, inverse, store_rows):
    tokens = activations.shape[0]
    rank = proj_in.shape[1]
    half = rank // cols
    docs = SLOTS * n // 2
    doc_rows = -(-docs // 16) * 16
    width = inverse.shape[1] // cols
    piece = SLOTS * half * rank // LANES // PARTS
    anywhere = pl.BlockSpec(memory_space=pl.ANY)
    dma = pltpu.SemaphoreType.DMA
    return pl.pallas_call(
        functools.partial(score_kernel, n, cols, docs),
        name="scores",
        out_shape=pltpu.VMEM((docs, store_rows.shape[0]), jnp.float32),
        in_specs=[anywhere] * 7,
        out_specs=pl.BlockSpec(memory_space=pltpu.VMEM),
        scratch_shapes=[
            pltpu.VMEM((tokens + rank, activations.shape[1]), jnp.bfloat16),
            pltpu.VMEM((tokens + rank, gradients.shape[1]), jnp.bfloat16),
            pltpu.VMEM(inverse.shape, jnp.float32),
            pltpu.VMEM(store_rows.shape, jnp.bfloat16),
            pltpu.VMEM(inverse.shape, jnp.bfloat16),
            pltpu.VMEM(inverse.shape, jnp.bfloat16),
            pltpu.VMEM(store_rows.shape[::-1], jnp.bfloat16),
            pltpu.VMEM((n, 1, tokens), jnp.int32),
            pltpu.VMEM((2 * half + rank, tokens), jnp.float32),
            pltpu.VMEM((2 * half + rank, tokens), jnp.float32),
            pltpu.VMEM((half, tokens), jnp.float32),
            pltpu.VMEM((PARTS, n * piece, LANES), jnp.float32),
            pltpu.VMEM((doc_rows, width), jnp.float32),
            pltpu.VMEM((doc_rows, width), jnp.float32),
            pltpu.VMEM((n * cols, doc_rows, width), jnp.bfloat16),
            dma((LEFT_CHUNKS + RIGHT_CHUNKS + 3,)),
            dma((5,)),
            dma((5 + PARTS,)),
        ],
        compiler_params=pltpu.CompilerParams(
            collective_id=0, has_side_effects=True, vmem_limit_bytes=60 << 20
        ),
    )(activations, gradients, doc_ids[None, :], proj_in.T, proj_out.T, inverse, store_rows)


def suits_kernel(n, cols, activations, gradients, proj_in, inverse):
    rank = proj_in.shape[1]
    return (
        cols == 2
        and activations.shape[0] == LANES
        and LANES % rank == 0
        and (rank // cols * rank) % (8 * PARTS * LANES) == 0
        and activations.shape[1] % (LEFT_CHUNKS * LANES) == 0
        and gradients.shape[1] % (RIGHT_CHUNKS * LANES) == 0
        and inverse.shape[1] % (cols * LANES) == 0
        and n <= 16
        and n & (n - 1) == 0
    )


def solution(mesh):
    in_specs = (
        P(("groups", "ctx"), "col"),
        P(("groups", "ctx"), "col"),
        P(("groups", "ctx")),
        P("col", None),
        P("col", None),
        P("col", "ctx"),
        P(("groups", "ctx", "col"), None),
    )
    out_specs = P(None, ("groups", "ctx", "col"))
    n, cols = mesh.shape["ctx"], mesh.shape["col"]

    def body(activations, gradients, doc_ids, proj_in, proj_out, inverse, store_rows):
        args = (activations, gradients, doc_ids, proj_in, proj_out, inverse, store_rows)
        if suits_kernel(n, cols, activations, gradients, proj_in, inverse):
            return fused(n, cols, *args)
        return shards(*args)

    return jax.shard_map(body, mesh=mesh, in_specs=in_specs, out_specs=out_specs, check_vma=False)
```

```python
import functools

import jax
import jax.numpy as jnp
from jax import lax
from jax.experimental import pallas as pl
from jax.experimental.pallas import tpu as pltpu
from jax.sharding import PartitionSpec as P


def from_behind(block, axis, distance):
    devices = range(lax.axis_size(axis))
    route = [(i - distance, i) for i in devices if i - distance in devices]
    return lax.ppermute(block, axis, route)


def shards(activations, gradients, doc_ids, proj_in, proj_out, inverse, store_rows):
    left_part = jnp.dot(activations, proj_in, preferred_element_type=jnp.float32)
    right_part = jnp.dot(gradients, proj_out, preferred_element_type=jnp.float32)
    proj_left, proj_right = lax.psum((left_part, right_part), "col")
    proj_rank = proj_right.shape[1]
    half_rank = proj_rank // lax.axis_size("col")
    own_half = lax.dynamic_slice_in_dim(proj_left, lax.axis_index("col") * half_rank, half_rank, 1)
    first_doc = doc_ids[0]
    slot_index = doc_ids - first_doc
    onehot = (slot_index[:, None] == jnp.arange(3, dtype=jnp.int32)[None, :]).astype(jnp.float32)
    weighted = (onehot[:, :, None] * own_half[:, None, :]).reshape(own_half.shape[0], 3 * half_rank)
    local_sums = lax.dot_general(
        weighted,
        proj_right,
        (((0,), (0,)), ((), ())),
        precision=lax.Precision.HIGHEST,
        preferred_element_type=jnp.float32,
    ).reshape(3, half_rank * proj_rank)
    doc_count = 3 * lax.axis_size("ctx") // 2
    last_row = lax.dynamic_index_in_dim(local_sums, slot_index[-1], 0, keepdims=False)
    incoming, incoming_id = from_behind((last_row, doc_ids[-1].astype(jnp.float32)), "ctx", 1)
    matches = (incoming_id == first_doc.astype(jnp.float32)).astype(jnp.float32)
    head_row = local_sums[0] + matches * incoming
    owned_rows = jnp.stack([head_row, local_sums[1]])
    owned_ids = (first_doc + jnp.arange(2, dtype=jnp.int32)).astype(jnp.float32)
    gathered, gathered_ids = (
        lax.all_gather(owned_rows, "ctx", axis=0, tiled=True),
        lax.all_gather(owned_ids, "ctx", axis=0, tiled=True),
    )
    positions = jnp.arange(gathered.shape[0], dtype=jnp.int32)
    wanted = jnp.arange(doc_count, dtype=jnp.int32).astype(jnp.float32)
    found = gathered_ids[None, :] == wanted[:, None]
    chosen = jnp.max(jnp.where(found, positions[None, :], -1), axis=1)
    doc_grads = jnp.take(gathered, chosen, axis=0)
    partial_q = jnp.dot(
        doc_grads, inverse, precision=lax.Precision.HIGHEST, preferred_element_type=jnp.float32
    )
    precond = lax.psum(partial_q, "col").astype(jnp.bfloat16)
    return lax.dot_general(
        lax.all_gather(precond, "ctx", axis=1, tiled=True),
        store_rows,
        (((1,), (1,)), ((), ())),
        preferred_element_type=jnp.float32,
    )


LANES = 128
ROWS = 8
SLOTS = 3
LEFT_CHUNKS = 1
RIGHT_CHUNKS = 4
MESH = pl.DeviceIdType.MESH
NT = (((1,), (1,)), ((), ()))


def halves(value):
    high = value.astype(jnp.bfloat16).astype(jnp.float32)
    return high, value - high


def dot_nt(left, right):
    return lax.dot_general(left, right, NT, preferred_element_type=jnp.float32)


def dot(left, right):
    return jnp.dot(left, right, preferred_element_type=jnp.float32)


def await_bytes(ref, sem):
    pltpu.make_async_copy(ref, ref, sem).wait()


def score_kernel(
    n, cols, docs,
    act, grad, ids, pin, pout, inv, store, out,
    xl, xr, inv_v, store_v, inv_hi, inv_lo, store_t, ids_v,
    part, came, full_l, notes, sums, q_part, q_from, q_all,
    load_sem, send_sem, recv_sem, ready,
):
    me = lax.axis_index("ctx")
    core = lax.axis_index("col")
    other = cols - 1 - core
    tokens = act.shape[0]
    rank = pin.shape[0]
    half = rank // cols
    pack = LANES // rank
    groups = half // pack
    piece = SLOTS * groups
    width = q_part.shape[1]
    spans = width // LANES

    def load(src, dst, sem):
        pltpu.make_async_copy(src, dst, load_sem.at[sem]).start()

    stages = []
    for x, w, v, count in ((act, pin, xl, LEFT_CHUNKS), (grad, pout, xr, RIGHT_CHUNKS)):
        step = x.shape[1] // count
        for i in range(count):
            span = pl.ds(i * step, step)
            load(x.at[:, span], v.at[pl.ds(0, tokens), span], len(stages))
            load(w.at[:, span], v.at[pl.ds(tokens, rank), span], len(stages))
            stages.append(v.at[:, span])
    ids_sem, inv_sem, store_sem = (len(stages) + i for i in range(3))
    load(ids, ids_v, ids_sem)
    load(inv, inv_v, inv_sem)
    load(store, store_v, store_sem)

    barrier = pltpu.get_barrier_semaphore()
    ctx_peers = [{"ctx": there} for there in far_first(me, n)]
    peers = [peer | {"col": to} for peer in ctx_peers for to in (core, other)]
    partner = {"col": other}

    @pl.when(core == cols - 1)
    def _():
        pl.semaphore_signal(barrier, inc=1, device_id=partner, device_id_type=MESH)

    for peer in ctx_peers:
        pl.semaphore_signal(barrier, inc=1, device_id=peer | {"col": cols - 1}, device_id_type=MESH)

    @pl.when(core == 0)
    def _():
        pl.semaphore_wait(barrier, 1)
        pl.semaphore_signal(ready, inc=1, device_id=partner, device_id_type=MESH)

    def send(src, dst, at, peer):
        pltpu.make_async_remote_copy(
            src_ref=src, dst_ref=dst, send_sem=send_sem.at[at], recv_sem=recv_sem.at[at],
            device_id=peer, device_id_type=MESH,
        ).start()

    totals = []
    for first, count in ((0, LEFT_CHUNKS), (LEFT_CHUNKS, RIGHT_CHUNKS)):
        total = None
        for i in range(first, first + count):
            await_bytes(stages[i], load_sem.at[i])
            v = stages[i]
            term = dot_nt(v[tokens:, :], v[:tokens, :])
            total = term if total is None else total + term
        totals.append(total)
    left, right = totals
    part[:half] = left[:half]
    part[half : half + rank] = right
    part[half + rank :] = left[half:]
    @pl.when(core == cols - 1)
    def _():
        pl.semaphore_wait(ready, 1)

    span = pl.ds(pl.multiple_of(other * half, half), half + rank)
    send(part.at[span], came.at[span], 0, partner)

    @pl.when(core == cols - 1)
    def _():
        pl.semaphore_wait(barrier, cols * (n - 1))
        pl.semaphore_signal(ready, inc=1, device_id=partner, device_id_type=MESH)

    await_bytes(ids_v, load_sem.at[ids_sem])
    own_ids = ids_v[...]
    first = own_ids[:, 0:1]
    masks = [(own_ids == first + s).astype(jnp.float32) for s in range(SLOTS)]
    await_bytes(part.at[pl.ds(0, half + rank)], recv_sem.at[0])
    rows = pl.ds(pl.multiple_of(core * (half + rank), half), half)
    full_l[...] = part[rows, :] + came[rows, :]
    highs, lows = [], []
    for p in range(pack):
        lines = full_l[pl.ds(p, groups, stride=pack), :]
        high, low = halves(jnp.concatenate([lines * mask for mask in masks], axis=0))
        highs.append(high)
        lows.append(low)
    weights = jnp.concatenate(highs + highs + lows, axis=1).astype(jnp.bfloat16)
    high, low = halves(part[half : half + rank] + came[half : half + rank])
    zero = jnp.zeros_like(high)

    def diagonal(block, p):
        return [block if q == p else zero for q in range(pack)]

    spread = jnp.concatenate(
        [
            jnp.concatenate(diagonal(high, p) + diagonal(low, p) + diagonal(high, p), axis=1)
            for p in range(pack)
        ],
        axis=0,
    ).astype(jnp.bfloat16)
    mine = pl.ds(pl.multiple_of(me * piece, ROWS), piece)
    notes[me] = jnp.broadcast_to(first, (1, LANES)).astype(jnp.float32)
    sums[mine, :] = dot_nt(weights, spread)

    @pl.when(core == 0)
    def _():
        pl.semaphore_wait(ready, 1)

    for peer in ctx_peers:
        send(notes.at[me], notes.at[me], 4, peer)
        send(sums.at[mine], sums.at[mine], 1, peer)

    await_bytes(inv_v, load_sem.at[inv_sem])
    band = LANES

    def split(i, carry):
        rows = pl.ds(pl.multiple_of(i * band, band), band)
        high, low = halves(inv_v[rows, :])
        inv_hi[rows, :] = high.astype(jnp.bfloat16)
        inv_lo[rows, :] = low.astype(jnp.bfloat16)
        return carry

    lax.fori_loop(0, inv_v.shape[0] // band, split, 0)
    await_bytes(store_v, load_sem.at[store_sem])
    stored = store_v.shape[0]
    for i in range(n * cols):
        tiles = []
        for j in range(spans):
            tile = (i * spans + j) * LANES
            tiles.append(store_v[:, tile : tile + LANES])
        store_t[i * LANES : (i + 1) * LANES, :] = jnp.concatenate(tiles, axis=0).T

    await_bytes(notes.at[pl.ds(0, n - 1)], recv_sem.at[4])
    await_bytes(sums.at[pl.ds(0, (n - 1) * piece)], recv_sem.at[1])
    gathered = jnp.concatenate(
        [sums[pl.ds(k, SLOTS * n, stride=groups), :] for k in range(groups)], axis=1
    )
    high, low = halves(gathered)
    both = jnp.concatenate([high, low], axis=0).astype(jnp.bfloat16)
    high = high.astype(jnp.bfloat16)
    doc_rows = q_part.shape[0]
    column = lax.broadcasted_iota(jnp.int32, (1, SLOTS * n), 1)
    doc_of = jnp.zeros((1, SLOTS * n), jnp.float32)
    for b in range(n):
        for s in range(SLOTS):
            doc_of = jnp.where(column == b * SLOTS + s, notes[b][:, :1] + s, doc_of)
    docs_at = lax.broadcasted_iota(jnp.int32, (doc_rows, SLOTS * n), 0).astype(jnp.float32)
    pick = (docs_at == doc_of).astype(jnp.bfloat16)
    pick = jnp.concatenate([pick, pick, pick], axis=1)

    def picked(side):
        at = pl.ds(pl.multiple_of(side * width, width), width)
        main = dot(both, inv_hi[:, at])
        rows = main[: SLOTS * n] + main[SLOTS * n :] + dot(high, inv_lo[:, at])
        high_rows, rest = halves(rows)
        middle, low_rows = halves(rest)
        return dot(pick, jnp.concatenate([high_rows, middle, low_rows], axis=0).astype(jnp.bfloat16))

    q_part[...] = picked(other)
    send(q_part, q_from, 2, partner)
    own = picked(core)
    await_bytes(q_part, recv_sem.at[2])
    slot = me * cols + core
    total = own + q_from[...]
    q_all[slot] = jnp.concatenate(
        [total[:docs, j * LANES : (j + 1) * LANES] for j in range(spans)], axis=0
    ).astype(jnp.bfloat16)
    for peer in peers + [partner]:
        send(q_all.at[slot], q_all.at[slot], 3, peer)
    await_bytes(q_all.at[pl.ds(0, n * cols - 1)], recv_sem.at[3])
    precond = jnp.concatenate([q_all[i] for i in range(n * cols)], axis=1)
    scores = dot(precond, store_t[...])
    out[...] = sum(scores[j * docs : (j + 1) * docs, j * stored : (j + 1) * stored] for j in range(spans))
    await_bytes(part.at[pl.ds(0, half + rank)], send_sem.at[0])
    await_bytes(sums.at[pl.ds(0, (n - 1) * piece)], send_sem.at[1])
    await_bytes(notes.at[pl.ds(0, n - 1)], send_sem.at[4])
    await_bytes(q_part, send_sem.at[2])
    await_bytes(q_all.at[pl.ds(0, n * cols - 1)], send_sem.at[3])


def far_first(me, n):
    rows = n // 2
    row, side = me // 2, me % 2
    upper = row >= rows // 2
    near = jnp.where(upper, rows - 1 - row, row)
    order = []
    for j in range(rows - 1):
        there = rows - 1 - j
        there = there - (there <= near).astype(jnp.int32)
        there = jnp.where(upper, rows - 1 - there, there)
        order += [2 * there + 1 - side, 2 * there + side]
    return order + [2 * row + 1 - side]


def fused(n, cols, activations, gradients, doc_ids, proj_in, proj_out, inverse, store_rows):
    tokens = activations.shape[0]
    rank = proj_in.shape[1]
    half = rank // cols
    docs = SLOTS * n // 2
    doc_rows = -(-docs // 16) * 16
    width = inverse.shape[1] // cols
    spans = width // LANES
    piece = SLOTS * half * rank // LANES
    anywhere = pl.BlockSpec(memory_space=pl.ANY)
    dma = pltpu.SemaphoreType.DMA
    return pl.pallas_call(
        functools.partial(score_kernel, n, cols, docs),
        name="scores",
        out_shape=pltpu.VMEM((docs, store_rows.shape[0]), jnp.float32),
        in_specs=[anywhere] * 7,
        out_specs=pl.BlockSpec(memory_space=pltpu.VMEM),
        scratch_shapes=[
            pltpu.VMEM((tokens + rank, activations.shape[1]), jnp.bfloat16),
            pltpu.VMEM((tokens + rank, gradients.shape[1]), jnp.bfloat16),
            pltpu.VMEM(inverse.shape, jnp.float32),
            pltpu.VMEM(store_rows.shape, jnp.bfloat16),
            pltpu.VMEM(inverse.shape, jnp.bfloat16),
            pltpu.VMEM(inverse.shape, jnp.bfloat16),
            pltpu.VMEM((store_rows.shape[1] // spans, spans * store_rows.shape[0]), jnp.bfloat16),
            pltpu.VMEM((1, tokens), jnp.int32),
            pltpu.VMEM((2 * half + rank, tokens), jnp.float32),
            pltpu.VMEM((2 * half + rank, tokens), jnp.float32),
            pltpu.VMEM((half, tokens), jnp.float32),
            pltpu.VMEM((n, 1, LANES), jnp.float32),
            pltpu.VMEM((n * piece, LANES), jnp.float32),
            pltpu.VMEM((doc_rows, width), jnp.float32),
            pltpu.VMEM((doc_rows, width), jnp.float32),
            pltpu.VMEM((n * cols, spans * docs, LANES), jnp.bfloat16),
            dma((LEFT_CHUNKS + RIGHT_CHUNKS + 3,)),
            dma((5,)),
            dma((5,)),
            pltpu.SemaphoreType.REGULAR,
        ],
        compiler_params=pltpu.CompilerParams(
            collective_id=0, has_side_effects=True, vmem_limit_bytes=60 << 20
        ),
    )(activations, gradients, doc_ids[None, :], proj_in.T, proj_out.T, inverse, store_rows)


def suits_kernel(n, cols, activations, gradients, proj_in, inverse):
    rank = proj_in.shape[1]
    return (
        cols == 2
        and activations.shape[0] == LANES
        and LANES % rank == 0
        and (rank // cols * rank) % (ROWS * LANES) == 0
        and activations.shape[1] % (LEFT_CHUNKS * LANES) == 0
        and gradients.shape[1] % (RIGHT_CHUNKS * LANES) == 0
        and inverse.shape[1] % (cols * LANES) == 0
        and 8 <= n <= 16
        and n & (n - 1) == 0
    )


def solution(mesh):
    in_specs = (
        P(("groups", "ctx"), "col"),
        P(("groups", "ctx"), "col"),
        P(("groups", "ctx")),
        P("col", None),
        P("col", None),
        P("col", "ctx"),
        P(("groups", "ctx", "col"), None),
    )
    out_specs = P(None, ("groups", "ctx", "col"))
    n, cols = mesh.shape["ctx"], mesh.shape["col"]

    def body(activations, gradients, doc_ids, proj_in, proj_out, inverse, store_rows):
        args = (activations, gradients, doc_ids, proj_in, proj_out, inverse, store_rows)
        if suits_kernel(n, cols, activations, gradients, proj_in, inverse):
            return fused(n, cols, *args)
        return shards(*args)

    return jax.shard_map(body, mesh=mesh, in_specs=in_specs, out_specs=out_specs, check_vma=False)
```

```python
import functools

import jax
import jax.numpy as jnp
from jax import lax
from jax.experimental import pallas as pl
from jax.experimental.pallas import tpu as pltpu
from jax.sharding import PartitionSpec as P


def from_behind(block, axis, distance):
    devices = range(lax.axis_size(axis))
    route = [(i - distance, i) for i in devices if i - distance in devices]
    return lax.ppermute(block, axis, route)


def shards(activations, gradients, doc_ids, proj_in, proj_out, inverse, store_rows):
    left_part = jnp.dot(activations, proj_in, preferred_element_type=jnp.float32)
    right_part = jnp.dot(gradients, proj_out, preferred_element_type=jnp.float32)
    proj_left, proj_right = lax.psum((left_part, right_part), "col")
    proj_rank = proj_right.shape[1]
    half_rank = proj_rank // lax.axis_size("col")
    own_half = lax.dynamic_slice_in_dim(proj_left, lax.axis_index("col") * half_rank, half_rank, 1)
    first_doc = doc_ids[0]
    slot_index = doc_ids - first_doc
    onehot = (slot_index[:, None] == jnp.arange(3, dtype=jnp.int32)[None, :]).astype(jnp.float32)
    weighted = (onehot[:, :, None] * own_half[:, None, :]).reshape(own_half.shape[0], 3 * half_rank)
    local_sums = lax.dot_general(
        weighted,
        proj_right,
        (((0,), (0,)), ((), ())),
        precision=lax.Precision.HIGHEST,
        preferred_element_type=jnp.float32,
    ).reshape(3, half_rank * proj_rank)
    doc_count = 3 * lax.axis_size("ctx") // 2
    last_row = lax.dynamic_index_in_dim(local_sums, slot_index[-1], 0, keepdims=False)
    incoming, incoming_id = from_behind((last_row, doc_ids[-1].astype(jnp.float32)), "ctx", 1)
    matches = (incoming_id == first_doc.astype(jnp.float32)).astype(jnp.float32)
    head_row = local_sums[0] + matches * incoming
    owned_rows = jnp.stack([head_row, local_sums[1]])
    owned_ids = (first_doc + jnp.arange(2, dtype=jnp.int32)).astype(jnp.float32)
    gathered, gathered_ids = (
        lax.all_gather(owned_rows, "ctx", axis=0, tiled=True),
        lax.all_gather(owned_ids, "ctx", axis=0, tiled=True),
    )
    positions = jnp.arange(gathered.shape[0], dtype=jnp.int32)
    wanted = jnp.arange(doc_count, dtype=jnp.int32).astype(jnp.float32)
    found = gathered_ids[None, :] == wanted[:, None]
    chosen = jnp.max(jnp.where(found, positions[None, :], -1), axis=1)
    doc_grads = jnp.take(gathered, chosen, axis=0)
    partial_q = jnp.dot(
        doc_grads, inverse, precision=lax.Precision.HIGHEST, preferred_element_type=jnp.float32
    )
    precond = lax.psum(partial_q, "col").astype(jnp.bfloat16)
    return lax.dot_general(
        lax.all_gather(precond, "ctx", axis=1, tiled=True),
        store_rows,
        (((1,), (1,)), ((), ())),
        preferred_element_type=jnp.float32,
    )


LANES = 128
ROWS = 8
SLOTS = 3
STEPS = 32767.0
LEAST = 2.0**-110
LEFT_CHUNKS = 1
RIGHT_CHUNKS = 4
MESH = pl.DeviceIdType.MESH
NT = (((1,), (1,)), ((), ()))


def halves(value):
    high = value.astype(jnp.bfloat16).astype(jnp.float32)
    return high, value - high


def dot_nt(left, right):
    return lax.dot_general(left, right, NT, preferred_element_type=jnp.float32)


def dot(left, right):
    return jnp.dot(left, right, preferred_element_type=jnp.float32)


def await_bytes(ref, sem):
    pltpu.make_async_copy(ref, ref, sem).wait()


def score_kernel(
    n, cols, docs,
    act, grad, ids, pin, pout, inv, store, out,
    xl, xr, inv_v, store_v, inv_hi, inv_lo, store_t, ids_v,
    part, came, full_l, codes, notes, sums, q_part, q_from, q_all,
    load_sem, send_sem, recv_sem, ready,
):
    me = lax.axis_index("ctx")
    core = lax.axis_index("col")
    other = cols - 1 - core
    tokens = act.shape[0]
    rank = pin.shape[0]
    half = rank // cols
    pack = LANES // rank
    groups = half // pack
    piece = SLOTS * groups
    width = q_part.shape[1]
    spans = width // LANES

    def load(src, dst, sem):
        pltpu.make_async_copy(src, dst, load_sem.at[sem]).start()

    stages = []
    for x, w, v, count in ((act, pin, xl, LEFT_CHUNKS), (grad, pout, xr, RIGHT_CHUNKS)):
        step = x.shape[1] // count
        for i in range(count):
            span = pl.ds(i * step, step)
            load(x.at[:, span], v.at[pl.ds(0, tokens), span], len(stages))
            load(w.at[:, span], v.at[pl.ds(tokens, rank), span], len(stages))
            stages.append(v.at[:, span])
    ids_sem, inv_sem, store_sem = (len(stages) + i for i in range(3))
    load(ids, ids_v, ids_sem)
    load(inv, inv_v, inv_sem)
    load(store, store_v, store_sem)

    barrier = pltpu.get_barrier_semaphore()
    ctx_peers = [{"ctx": there} for there in far_first(me, n)]
    peers = [peer | {"col": to} for peer in ctx_peers for to in (core, other)]
    partner = {"col": other}

    @pl.when(core == cols - 1)
    def _():
        pl.semaphore_signal(barrier, inc=1, device_id=partner, device_id_type=MESH)

    for peer in ctx_peers:
        pl.semaphore_signal(barrier, inc=1, device_id=peer | {"col": cols - 1}, device_id_type=MESH)

    @pl.when(core == 0)
    def _():
        pl.semaphore_wait(barrier, 1)
        pl.semaphore_signal(ready, inc=1, device_id=partner, device_id_type=MESH)

    def send(src, dst, at, peer):
        pltpu.make_async_remote_copy(
            src_ref=src, dst_ref=dst, send_sem=send_sem.at[at], recv_sem=recv_sem.at[at],
            device_id=peer, device_id_type=MESH,
        ).start()

    totals = []
    for first, count in ((0, LEFT_CHUNKS), (LEFT_CHUNKS, RIGHT_CHUNKS)):
        total = None
        for i in range(first, first + count):
            await_bytes(stages[i], load_sem.at[i])
            v = stages[i]
            term = dot_nt(v[tokens:, :], v[:tokens, :])
            total = term if total is None else total + term
        totals.append(total)
    left, right = totals
    part[:half] = left[:half]
    part[half : half + rank] = right
    part[half + rank :] = left[half:]
    @pl.when(core == cols - 1)
    def _():
        pl.semaphore_wait(ready, 1)

    span = pl.ds(pl.multiple_of(other * half, half), half + rank)
    send(part.at[span], came.at[span], 0, partner)

    @pl.when(core == cols - 1)
    def _():
        pl.semaphore_wait(barrier, cols * (n - 1))
        pl.semaphore_signal(ready, inc=1, device_id=partner, device_id_type=MESH)

    await_bytes(ids_v, load_sem.at[ids_sem])
    own_ids = ids_v[...]
    first = own_ids[:, 0:1]
    masks = [(own_ids == first + s).astype(jnp.float32) for s in range(SLOTS)]
    await_bytes(part.at[pl.ds(0, half + rank)], recv_sem.at[0])
    rows = pl.ds(pl.multiple_of(core * (half + rank), half), half)
    full_l[...] = part[rows, :] + came[rows, :]
    highs, lows = [], []
    for p in range(pack):
        lines = full_l[pl.ds(p, groups, stride=pack), :]
        high, low = halves(jnp.concatenate([lines * mask for mask in masks], axis=0))
        highs.append(high)
        lows.append(low)
    weights = jnp.concatenate(highs + highs + lows, axis=1).astype(jnp.bfloat16)
    high, low = halves(part[half : half + rank] + came[half : half + rank])
    zero = jnp.zeros_like(high)

    def diagonal(block, p):
        return [block if q == p else zero for q in range(pack)]

    spread = jnp.concatenate(
        [
            jnp.concatenate(diagonal(high, p) + diagonal(low, p) + diagonal(high, p), axis=1)
            for p in range(pack)
        ],
        axis=0,
    ).astype(jnp.bfloat16)
    mine = pl.ds(pl.multiple_of(me * piece, 2 * ROWS), piece)
    product = dot_nt(weights, spread)
    lane = lax.broadcasted_iota(jnp.int32, (1, LANES), 1)
    note = jnp.broadcast_to(first.astype(jnp.float32), (1, LANES))
    coded = []
    for s in range(SLOTS):
        rows_s = product[s * groups : (s + 1) * groups]
        top = jnp.max(jnp.max(jnp.abs(rows_s), axis=0, keepdims=True), axis=1, keepdims=True)
        top = jnp.maximum(top, LEAST)
        coded.append(jnp.floor(rows_s * (STEPS / top) + 0.5))
        note = jnp.where(lane > s, top * (1.0 / STEPS), note)
    notes[me] = note
    codes[mine, :] = jnp.concatenate(coded, axis=0).astype(jnp.int32).astype(jnp.int16)

    @pl.when(core == 0)
    def _():
        pl.semaphore_wait(ready, 1)

    for peer in ctx_peers:
        send(notes.at[me], notes.at[me], 4, peer)
        send(codes.at[mine], codes.at[mine], 1, peer)

    await_bytes(inv_v, load_sem.at[inv_sem])
    band = LANES

    def split(i, carry):
        rows = pl.ds(pl.multiple_of(i * band, band), band)
        high, low = halves(inv_v[rows, :])
        inv_hi[rows, :] = high.astype(jnp.bfloat16)
        inv_lo[rows, :] = low.astype(jnp.bfloat16)
        return carry

    lax.fori_loop(0, inv_v.shape[0] // band, split, 0)
    await_bytes(store_v, load_sem.at[store_sem])
    stored = store_v.shape[0]
    for i in range(n * cols):
        tiles = []
        for j in range(spans):
            tile = (i * spans + j) * LANES
            tiles.append(store_v[:, tile : tile + LANES])
        store_t[i * LANES : (i + 1) * LANES, :] = jnp.concatenate(tiles, axis=0).T

    await_bytes(notes.at[pl.ds(0, n - 1)], recv_sem.at[4])
    await_bytes(codes.at[pl.ds(0, (n - 1) * piece)], recv_sem.at[1])
    for b in range(n):
        for s in range(SLOTS):
            at = slice(b * piece + s * groups, b * piece + (s + 1) * groups)
            sums[at] = codes[at].astype(jnp.int32).astype(jnp.float32) * notes[b][:, s + 1 : s + 2]
    gathered = jnp.concatenate(
        [sums[pl.ds(k, SLOTS * n, stride=groups), :] for k in range(groups)], axis=1
    )
    high, low = halves(gathered)
    both = jnp.concatenate([high, low], axis=0).astype(jnp.bfloat16)
    high = high.astype(jnp.bfloat16)
    doc_rows = q_part.shape[0]
    column = lax.broadcasted_iota(jnp.int32, (1, SLOTS * n), 1)
    doc_of = jnp.zeros((1, SLOTS * n), jnp.float32)
    for b in range(n):
        for s in range(SLOTS):
            doc_of = jnp.where(column == b * SLOTS + s, notes[b][:, :1] + s, doc_of)
    docs_at = lax.broadcasted_iota(jnp.int32, (doc_rows, SLOTS * n), 0).astype(jnp.float32)
    pick = (docs_at == doc_of).astype(jnp.bfloat16)
    pick = jnp.concatenate([pick, pick, pick], axis=1)

    def picked(side):
        at = pl.ds(pl.multiple_of(side * width, width), width)
        main = dot(both, inv_hi[:, at])
        rows = main[: SLOTS * n] + main[SLOTS * n :] + dot(high, inv_lo[:, at])
        high_rows, rest = halves(rows)
        middle, low_rows = halves(rest)
        return dot(pick, jnp.concatenate([high_rows, middle, low_rows], axis=0).astype(jnp.bfloat16))

    q_part[...] = picked(other)
    send(q_part, q_from, 2, partner)
    own = picked(core)
    await_bytes(q_part, recv_sem.at[2])
    slot = me * cols + core
    total = own + q_from[...]
    q_all[slot] = jnp.concatenate(
        [total[:docs, j * LANES : (j + 1) * LANES] for j in range(spans)], axis=0
    ).astype(jnp.bfloat16)
    for peer in peers + [partner]:
        send(q_all.at[slot], q_all.at[slot], 3, peer)
    await_bytes(q_all.at[pl.ds(0, n * cols - 1)], recv_sem.at[3])
    precond = jnp.concatenate([q_all[i] for i in range(n * cols)], axis=1)
    scores = dot(precond, store_t[...])
    out[...] = sum(scores[j * docs : (j + 1) * docs, j * stored : (j + 1) * stored] for j in range(spans))
    await_bytes(part.at[pl.ds(0, half + rank)], send_sem.at[0])
    await_bytes(codes.at[pl.ds(0, (n - 1) * piece)], send_sem.at[1])
    await_bytes(notes.at[pl.ds(0, n - 1)], send_sem.at[4])
    await_bytes(q_part, send_sem.at[2])
    await_bytes(q_all.at[pl.ds(0, n * cols - 1)], send_sem.at[3])


def far_first(me, n):
    rows = n // 2
    row, side = me // 2, me % 2
    upper = row >= rows // 2
    near = jnp.where(upper, rows - 1 - row, row)
    order = []
    for j in range(rows - 1):
        there = rows - 1 - j
        there = there - (there <= near).astype(jnp.int32)
        there = jnp.where(upper, rows - 1 - there, there)
        order += [2 * there + 1 - side, 2 * there + side]
    return order + [2 * row + 1 - side]


def fused(n, cols, activations, gradients, doc_ids, proj_in, proj_out, inverse, store_rows):
    tokens = activations.shape[0]
    rank = proj_in.shape[1]
    half = rank // cols
    docs = SLOTS * n // 2
    doc_rows = -(-docs // 16) * 16
    width = inverse.shape[1] // cols
    spans = width // LANES
    piece = SLOTS * half * rank // LANES
    anywhere = pl.BlockSpec(memory_space=pl.ANY)
    dma = pltpu.SemaphoreType.DMA
    return pl.pallas_call(
        functools.partial(score_kernel, n, cols, docs),
        name="scores",
        out_shape=pltpu.VMEM((docs, store_rows.shape[0]), jnp.float32),
        in_specs=[anywhere] * 7,
        out_specs=pl.BlockSpec(memory_space=pltpu.VMEM),
        scratch_shapes=[
            pltpu.VMEM((tokens + rank, activations.shape[1]), jnp.bfloat16),
            pltpu.VMEM((tokens + rank, gradients.shape[1]), jnp.bfloat16),
            pltpu.VMEM(inverse.shape, jnp.float32),
            pltpu.VMEM(store_rows.shape, jnp.bfloat16),
            pltpu.VMEM(inverse.shape, jnp.bfloat16),
            pltpu.VMEM(inverse.shape, jnp.bfloat16),
            pltpu.VMEM((store_rows.shape[1] // spans, spans * store_rows.shape[0]), jnp.bfloat16),
            pltpu.VMEM((1, tokens), jnp.int32),
            pltpu.VMEM((2 * half + rank, tokens), jnp.float32),
            pltpu.VMEM((2 * half + rank, tokens), jnp.float32),
            pltpu.VMEM((half, tokens), jnp.float32),
            pltpu.VMEM((n * piece, LANES), jnp.int16),
            pltpu.VMEM((n, 1, LANES), jnp.float32),
            pltpu.VMEM((n * piece, LANES), jnp.float32),
            pltpu.VMEM((doc_rows, width), jnp.float32),
            pltpu.VMEM((doc_rows, width), jnp.float32),
            pltpu.VMEM((n * cols, spans * docs, LANES), jnp.bfloat16),
            dma((LEFT_CHUNKS + RIGHT_CHUNKS + 3,)),
            dma((5,)),
            dma((5,)),
            pltpu.SemaphoreType.REGULAR,
        ],
        compiler_params=pltpu.CompilerParams(
            collective_id=0, has_side_effects=True, vmem_limit_bytes=60 << 20
        ),
    )(activations, gradients, doc_ids[None, :], proj_in.T, proj_out.T, inverse, store_rows)


def suits_kernel(n, cols, activations, gradients, proj_in, inverse):
    rank = proj_in.shape[1]
    return (
        cols == 2
        and activations.shape[0] == LANES
        and LANES % rank == 0
        and (rank // cols * rank) % (ROWS * LANES) == 0
        and activations.shape[1] % (LEFT_CHUNKS * LANES) == 0
        and gradients.shape[1] % (RIGHT_CHUNKS * LANES) == 0
        and inverse.shape[1] % (cols * LANES) == 0
        and 8 <= n <= 16
        and n & (n - 1) == 0
    )


def solution(mesh):
    in_specs = (
        P(("groups", "ctx"), "col"),
        P(("groups", "ctx"), "col"),
        P(("groups", "ctx")),
        P("col", None),
        P("col", None),
        P("col", "ctx"),
        P(("groups", "ctx", "col"), None),
    )
    out_specs = P(None, ("groups", "ctx", "col"))
    n, cols = mesh.shape["ctx"], mesh.shape["col"]

    def body(activations, gradients, doc_ids, proj_in, proj_out, inverse, store_rows):
        args = (activations, gradients, doc_ids, proj_in, proj_out, inverse, store_rows)
        if suits_kernel(n, cols, activations, gradients, proj_in, inverse):
            return fused(n, cols, *args)
        return shards(*args)

    return jax.shard_map(body, mesh=mesh, in_specs=in_specs, out_specs=out_specs, check_vma=False)
```

```python
import functools

import jax
import jax.numpy as jnp
from jax import lax
from jax.experimental import pallas as pl
from jax.experimental.pallas import tpu as pltpu
from jax.sharding import PartitionSpec as P


def from_behind(block, axis, distance):
    devices = range(lax.axis_size(axis))
    route = [(i - distance, i) for i in devices if i - distance in devices]
    return lax.ppermute(block, axis, route)


def shards(activations, gradients, doc_ids, proj_in, proj_out, inverse, store_rows):
    left_part = jnp.dot(activations, proj_in, preferred_element_type=jnp.float32)
    right_part = jnp.dot(gradients, proj_out, preferred_element_type=jnp.float32)
    proj_left, proj_right = lax.psum((left_part, right_part), "col")
    proj_rank = proj_right.shape[1]
    half_rank = proj_rank // lax.axis_size("col")
    own_half = lax.dynamic_slice_in_dim(proj_left, lax.axis_index("col") * half_rank, half_rank, 1)
    first_doc = doc_ids[0]
    slot_index = doc_ids - first_doc
    onehot = (slot_index[:, None] == jnp.arange(3, dtype=jnp.int32)[None, :]).astype(jnp.float32)
    weighted = (onehot[:, :, None] * own_half[:, None, :]).reshape(own_half.shape[0], 3 * half_rank)
    local_sums = lax.dot_general(
        weighted,
        proj_right,
        (((0,), (0,)), ((), ())),
        precision=lax.Precision.HIGHEST,
        preferred_element_type=jnp.float32,
    ).reshape(3, half_rank * proj_rank)
    doc_count = 3 * lax.axis_size("ctx") // 2
    last_row = lax.dynamic_index_in_dim(local_sums, slot_index[-1], 0, keepdims=False)
    incoming, incoming_id = from_behind((last_row, doc_ids[-1].astype(jnp.float32)), "ctx", 1)
    matches = (incoming_id == first_doc.astype(jnp.float32)).astype(jnp.float32)
    head_row = local_sums[0] + matches * incoming
    owned_rows = jnp.stack([head_row, local_sums[1]])
    owned_ids = (first_doc + jnp.arange(2, dtype=jnp.int32)).astype(jnp.float32)
    gathered, gathered_ids = (
        lax.all_gather(owned_rows, "ctx", axis=0, tiled=True),
        lax.all_gather(owned_ids, "ctx", axis=0, tiled=True),
    )
    positions = jnp.arange(gathered.shape[0], dtype=jnp.int32)
    wanted = jnp.arange(doc_count, dtype=jnp.int32).astype(jnp.float32)
    found = gathered_ids[None, :] == wanted[:, None]
    chosen = jnp.max(jnp.where(found, positions[None, :], -1), axis=1)
    doc_grads = jnp.take(gathered, chosen, axis=0)
    partial_q = jnp.dot(
        doc_grads, inverse, precision=lax.Precision.HIGHEST, preferred_element_type=jnp.float32
    )
    precond = lax.psum(partial_q, "col").astype(jnp.bfloat16)
    return lax.dot_general(
        lax.all_gather(precond, "ctx", axis=1, tiled=True),
        store_rows,
        (((1,), (1,)), ((), ())),
        preferred_element_type=jnp.float32,
    )


LANES = 128
ROWS = 8
SLOTS = 3
STEPS = 32767.0
LEAST = 2.0**-110
LEFT_CHUNKS = 1
RIGHT_CHUNKS = 4
MESH = pl.DeviceIdType.MESH
NT = (((1,), (1,)), ((), ()))


def halves(value):
    high = value.astype(jnp.bfloat16).astype(jnp.float32)
    return high, value - high


def dot_nt(left, right):
    return lax.dot_general(left, right, NT, preferred_element_type=jnp.float32)


def dot(left, right):
    return jnp.dot(left, right, preferred_element_type=jnp.float32)


def await_bytes(ref, sem):
    pltpu.make_async_copy(ref, ref, sem).wait()


def score_kernel(
    n, cols, docs,
    act, grad, ids, pin, pout, inv, store, out,
    xl, xr, inv_v, store_v, inv_hi, inv_lo, store_t, ids_v,
    part, came, full_l, codes, notes, tally, sums, q_part, q_from, q_all,
    load_sem, send_sem, recv_sem, ready,
):
    me = lax.axis_index("ctx")
    core = lax.axis_index("col")
    other = cols - 1 - core
    tokens = act.shape[0] * ROWS
    rank = pin.shape[0] * ROWS
    half = rank // cols
    pack = LANES // rank
    groups = half // pack
    piece = SLOTS * groups
    width = q_part.shape[1]
    spans = width // LANES

    barrier = pltpu.get_barrier_semaphore()
    ctx_peers = [{"ctx": there} for there in far_first(me, n)]
    peers = [peer | {"col": to} for peer in ctx_peers for to in (core, other)]
    partner = {"col": other}

    @pl.when(core == cols - 1)
    def _():
        pl.semaphore_signal(barrier, inc=1, device_id=partner, device_id_type=MESH)

    for peer in ctx_peers:
        pl.semaphore_signal(barrier, inc=1, device_id=peer | {"col": cols - 1}, device_id_type=MESH)

    def load(src, dst, sem):
        pltpu.make_async_copy(src, dst, load_sem.at[sem]).start()

    stages = []
    for x, w, v, count in ((act, pin, xl, LEFT_CHUNKS), (grad, pout, xr, RIGHT_CHUNKS)):
        step = x.shape[1] // count
        for i in range(count):
            span = pl.ds(i * step, step)
            for source, row in ((x, 0), (w, tokens)):
                for j in range(source.shape[0]):
                    load(source.at[j, span], v.at[span, pl.ds(row + j * ROWS, ROWS)], len(stages))
            stages.append(v.at[span])
    ids_sem, inv_sem, store_sem = (len(stages) + i for i in range(3))
    load(ids, ids_v, ids_sem)
    load(inv, inv_v, inv_sem)
    load(store, store_v, store_sem)

    @pl.when(core == 0)
    def _():
        pl.semaphore_wait(barrier, 1)
        pl.semaphore_signal(ready, inc=1, device_id=partner, device_id_type=MESH)

    def send(src, dst, at, peer):
        pltpu.make_async_remote_copy(
            src_ref=src, dst_ref=dst, send_sem=send_sem.at[0], recv_sem=recv_sem.at[at],
            device_id=peer, device_id_type=MESH,
        ).start()

    totals = []
    for first, count in ((0, LEFT_CHUNKS), (LEFT_CHUNKS, RIGHT_CHUNKS)):
        total = None
        for i in range(first, first + count):
            await_bytes(stages[i], load_sem.at[i])
            tiles = stages[i].shape[0]
            cuts = 2 if i >= LEFT_CHUNKS + RIGHT_CHUNKS - 2 else 1
            terms = []
            for c in range(cuts):
                deep = jnp.concatenate(
                    [stages[i][k] for k in range(c * tiles // cuts, (c + 1) * tiles // cuts)], axis=1
                )
                terms.append(dot_nt(deep[tokens:], deep[:tokens]))
            term = sum(terms[1:], terms[0])
            total = term if total is None else total + term
        totals.append(total)
    left, right = totals
    part[:half] = left[:half]
    part[half : half + rank] = right
    part[half + rank :] = left[half:]
    @pl.when(core == cols - 1)
    def _():
        pl.semaphore_wait(ready, 1)

    span = pl.ds(pl.multiple_of(other * half, half), half + rank)
    send(part.at[span], came.at[span], 0, partner)

    @pl.when(core == cols - 1)
    def _():
        pl.semaphore_wait(barrier, cols * (n - 1))
        pl.semaphore_signal(ready, inc=1, device_id=partner, device_id_type=MESH)

    await_bytes(ids_v, load_sem.at[ids_sem])
    own_ids = ids_v[...]
    first = own_ids[:, 0:1]
    masks = [(own_ids == first + s).astype(jnp.float32) for s in range(SLOTS)]
    await_bytes(part.at[pl.ds(0, half + rank)], recv_sem.at[0])
    rows = pl.ds(pl.multiple_of(core * (half + rank), half), half)
    full_l[...] = part[rows, :] + came[rows, :]
    highs, lows = [], []
    for p in range(pack):
        lines = full_l[pl.ds(p, groups, stride=pack), :]
        high, low = halves(jnp.concatenate([lines * mask for mask in masks], axis=0))
        highs.append(high)
        lows.append(low)
    weights = jnp.concatenate(highs + highs + lows, axis=1).astype(jnp.bfloat16)
    high, low = halves(part[half : half + rank] + came[half : half + rank])
    zero = jnp.zeros_like(high)

    def diagonal(block, p):
        return [block if q == p else zero for q in range(pack)]

    spread = jnp.concatenate(
        [
            jnp.concatenate(diagonal(high, p) + diagonal(low, p) + diagonal(high, p), axis=1)
            for p in range(pack)
        ],
        axis=0,
    ).astype(jnp.bfloat16)
    mine = pl.ds(pl.multiple_of(me * piece, 2 * ROWS), piece)
    product = dot_nt(weights, spread)
    lane = lax.broadcasted_iota(jnp.int32, (1, LANES), 1)
    note = jnp.broadcast_to(first.astype(jnp.float32), (1, LANES))
    coded = []
    for s in range(SLOTS):
        rows_s = product[s * groups : (s + 1) * groups]
        top = jnp.max(jnp.max(jnp.abs(rows_s), axis=0, keepdims=True), axis=1, keepdims=True)
        top = jnp.maximum(top, LEAST)
        coded.append(jnp.floor(rows_s * (STEPS / top) + 0.5))
        note = jnp.where(lane > s, top * (1.0 / STEPS), note)
    notes[me] = note
    codes[mine, :] = jnp.concatenate(coded, axis=0).astype(jnp.int32).astype(jnp.int16)

    @pl.when(core == 0)
    def _():
        pl.semaphore_wait(ready, 1)

    for peer in ctx_peers:
        wave = 1 + 3 * (jnp.bitwise_xor(me, peer["ctx"]) // 2 % 2)
        send(notes.at[me], notes.at[me], wave, peer)
        send(codes.at[mine], codes.at[mine], wave, peer)

    await_bytes(inv_v, load_sem.at[inv_sem])
    band = LANES

    def split(i, carry):
        rows = pl.ds(pl.multiple_of(i * band, band), band)
        high, low = halves(inv_v[rows, :])
        inv_hi[rows, :] = high.astype(jnp.bfloat16)
        inv_lo[rows, :] = low.astype(jnp.bfloat16)
        return carry

    lax.fori_loop(0, inv_v.shape[0] // band, split, 0)
    await_bytes(store_v, load_sem.at[store_sem])
    stored = store_v.shape[0]
    for i in range(n * cols):
        tiles = []
        for j in range(spans):
            tile = (i * spans + j) * LANES
            tiles.append(store_v[:, tile : tile + LANES])
        store_t[i * LANES : (i + 1) * LANES, :] = jnp.concatenate(tiles, axis=0).T

    def decode(r):
        there = jnp.bitwise_xor(me, r)
        note = notes[there]
        block = codes[pl.ds(pl.multiple_of(there * piece, 2 * ROWS), piece), :].astype(jnp.int32).astype(jnp.float32)
        for s in range(SLOTS):
            rows = block[s * groups : (s + 1) * groups] * note[:, s + 1 : s + 2]
            sums[pl.ds(r * SLOTS + s, groups, stride=SLOTS * n), :] = rows

    decode(0)
    for wave, senders in ((4, n // 2), (1, n // 2 - 1)):
        await_bytes(tally.at[pl.ds(0, senders * (1 + piece // 2))], recv_sem.at[wave])
        for r in range(1, n):
            if (r // 2 % 2 == 1) == (wave == 4):
                decode(r)
    gathered = jnp.concatenate(
        [sums[k * SLOTS * n : (k + 1) * SLOTS * n, :] for k in range(groups)], axis=1
    )
    high, low = halves(gathered)
    both = jnp.concatenate([high, low], axis=0).astype(jnp.bfloat16)
    high = high.astype(jnp.bfloat16)
    doc_rows = q_part.shape[0]
    column = lax.broadcasted_iota(jnp.int32, (1, SLOTS * n), 1)
    doc_of = jnp.zeros((1, SLOTS * n), jnp.float32)
    for r in range(n):
        for s in range(SLOTS):
            doc_of = jnp.where(column == r * SLOTS + s, notes[jnp.bitwise_xor(me, r)][:, :1] + s, doc_of)
    docs_at = lax.broadcasted_iota(jnp.int32, (doc_rows, SLOTS * n), 0).astype(jnp.float32)
    pick = (docs_at == doc_of).astype(jnp.bfloat16)
    pick = jnp.concatenate([pick, pick, pick], axis=1)

    def picked(side):
        at = pl.ds(pl.multiple_of(side * width, width), width)
        main = dot(both, inv_hi[:, at])
        rows = main[: SLOTS * n] + main[SLOTS * n :] + dot(high, inv_lo[:, at])
        high_rows, rest = halves(rows)
        middle, low_rows = halves(rest)
        return dot(pick, jnp.concatenate([high_rows, middle, low_rows], axis=0).astype(jnp.bfloat16))

    q_part[...] = picked(other)
    send(q_part, q_from, 2, partner)
    own = picked(core)
    await_bytes(q_part, recv_sem.at[2])
    slot = me * cols + core
    total = own + q_from[...]
    q_all[slot] = jnp.concatenate(
        [total[:docs, j * LANES : (j + 1) * LANES] for j in range(spans)], axis=0
    ).astype(jnp.bfloat16)
    for peer in peers + [partner]:
        send(q_all.at[slot], q_all.at[slot], 3, peer)
    await_bytes(q_all.at[pl.ds(0, n * cols - 1)], recv_sem.at[3])
    precond = jnp.concatenate([q_all[i] for i in range(n * cols)], axis=1)
    scores = dot(precond, store_t[...])
    out[...] = sum(scores[j * docs : (j + 1) * docs, j * stored : (j + 1) * stored] for j in range(spans))
    await_bytes(tally, send_sem.at[0])


def far_first(me, n):
    rows = n // 2
    row, side = me // 2, me % 2
    upper = row >= rows // 2
    near = jnp.where(upper, rows - 1 - row, row)
    order = []
    for j in range(rows - 1):
        there = rows - 1 - j
        there = there - (there <= near).astype(jnp.int32)
        there = jnp.where(upper, rows - 1 - there, there)
        order += [2 * there + 1 - side, 2 * there + side]
    return order[:2] + [2 * row + 1 - side] + order[2:]


def tiled(x):
    rows, columns = x.shape
    return x.reshape(rows // ROWS, ROWS, columns // LANES, LANES).transpose(0, 2, 1, 3)


def fused(n, cols, activations, gradients, doc_ids, proj_in, proj_out, inverse, store_rows):
    tokens = activations.shape[0]
    rank = proj_in.shape[1]
    half = rank // cols
    docs = SLOTS * n // 2
    doc_rows = -(-docs // 16) * 16
    width = inverse.shape[1] // cols
    spans = width // LANES
    piece = SLOTS * half * rank // LANES
    sent = 4 * (half + rank) * tokens + (n - 1) * (4 + 2 * piece) * LANES + 4 * doc_rows * width
    sent += (n * cols - 1) * 2 * spans * docs * LANES
    anywhere = pl.BlockSpec(memory_space=pl.ANY)
    dma = pltpu.SemaphoreType.DMA
    return pl.pallas_call(
        functools.partial(score_kernel, n, cols, docs),
        name="scores",
        out_shape=pltpu.VMEM((docs, store_rows.shape[0]), jnp.float32),
        in_specs=[anywhere] * 7,
        out_specs=pl.BlockSpec(memory_space=pltpu.VMEM),
        scratch_shapes=[
            pltpu.VMEM((activations.shape[1] // LANES, tokens + rank, LANES), jnp.bfloat16),
            pltpu.VMEM((gradients.shape[1] // LANES, tokens + rank, LANES), jnp.bfloat16),
            pltpu.VMEM(inverse.shape, jnp.float32),
            pltpu.VMEM(store_rows.shape, jnp.bfloat16),
            pltpu.VMEM(inverse.shape, jnp.bfloat16),
            pltpu.VMEM(inverse.shape, jnp.bfloat16),
            pltpu.VMEM((store_rows.shape[1] // spans, spans * store_rows.shape[0]), jnp.bfloat16),
            pltpu.VMEM((1, tokens), jnp.int32),
            pltpu.VMEM((2 * half + rank, tokens), jnp.float32),
            pltpu.VMEM((2 * half + rank, tokens), jnp.float32),
            pltpu.VMEM((half, tokens), jnp.float32),
            pltpu.VMEM((n * piece, LANES), jnp.int16),
            pltpu.VMEM((n, 1, LANES), jnp.float32),
            pltpu.VMEM((sent // (4 * LANES), 1, LANES), jnp.float32),
            pltpu.VMEM((n * piece, LANES), jnp.float32),
            pltpu.VMEM((doc_rows, width), jnp.float32),
            pltpu.VMEM((doc_rows, width), jnp.float32),
            pltpu.VMEM((n * cols, spans * docs, LANES), jnp.bfloat16),
            dma((LEFT_CHUNKS + RIGHT_CHUNKS + 3,)),
            dma((1,)),
            dma((5,)),
            pltpu.SemaphoreType.REGULAR,
        ],
        compiler_params=pltpu.CompilerParams(
            collective_id=0, has_side_effects=True, vmem_limit_bytes=60 << 20
        ),
    )(tiled(activations), tiled(gradients), doc_ids[None, :], tiled(proj_in.T), tiled(proj_out.T), inverse, store_rows)


def suits_kernel(n, cols, activations, gradients, proj_in, inverse):
    rank = proj_in.shape[1]
    return (
        cols == 2
        and activations.shape[0] == LANES
        and LANES % rank == 0
        and (rank // cols * rank) % (ROWS * LANES) == 0
        and activations.shape[1] % (LEFT_CHUNKS * LANES) == 0
        and gradients.shape[1] % (RIGHT_CHUNKS * LANES) == 0
        and inverse.shape[1] % (cols * LANES) == 0
        and 8 <= n <= 16
        and n & (n - 1) == 0
    )


def solution(mesh):
    in_specs = (
        P(("groups", "ctx"), "col"),
        P(("groups", "ctx"), "col"),
        P(("groups", "ctx")),
        P("col", None),
        P("col", None),
        P("col", "ctx"),
        P(("groups", "ctx", "col"), None),
    )
    out_specs = P(None, ("groups", "ctx", "col"))
    n, cols = mesh.shape["ctx"], mesh.shape["col"]

    def body(activations, gradients, doc_ids, proj_in, proj_out, inverse, store_rows):
        args = (activations, gradients, doc_ids, proj_in, proj_out, inverse, store_rows)
        if suits_kernel(n, cols, activations, gradients, proj_in, inverse):
            return fused(n, cols, *args)
        return shards(*args)

    return jax.shard_map(body, mesh=mesh, in_specs=in_specs, out_specs=out_specs, check_vma=False)
```

```python
import functools

import jax
import jax.numpy as jnp
from jax import lax
from jax.experimental import pallas as pl
from jax.experimental.pallas import tpu as pltpu
from jax.sharding import PartitionSpec as P


def from_behind(block, axis, distance):
    devices = range(lax.axis_size(axis))
    route = [(i - distance, i) for i in devices if i - distance in devices]
    return lax.ppermute(block, axis, route)


def shards(activations, gradients, doc_ids, proj_in, proj_out, inverse, store_rows):
    left_part = jnp.dot(activations, proj_in, preferred_element_type=jnp.float32)
    right_part = jnp.dot(gradients, proj_out, preferred_element_type=jnp.float32)
    proj_left, proj_right = lax.psum((left_part, right_part), "col")
    proj_rank = proj_right.shape[1]
    half_rank = proj_rank // lax.axis_size("col")
    own_half = lax.dynamic_slice_in_dim(proj_left, lax.axis_index("col") * half_rank, half_rank, 1)
    first_doc = doc_ids[0]
    slot_index = doc_ids - first_doc
    onehot = (slot_index[:, None] == jnp.arange(3, dtype=jnp.int32)[None, :]).astype(jnp.float32)
    weighted = (onehot[:, :, None] * own_half[:, None, :]).reshape(own_half.shape[0], 3 * half_rank)
    local_sums = lax.dot_general(
        weighted,
        proj_right,
        (((0,), (0,)), ((), ())),
        precision=lax.Precision.HIGHEST,
        preferred_element_type=jnp.float32,
    ).reshape(3, half_rank * proj_rank)
    doc_count = 3 * lax.axis_size("ctx") // 2
    last_row = lax.dynamic_index_in_dim(local_sums, slot_index[-1], 0, keepdims=False)
    incoming, incoming_id = from_behind((last_row, doc_ids[-1].astype(jnp.float32)), "ctx", 1)
    matches = (incoming_id == first_doc.astype(jnp.float32)).astype(jnp.float32)
    head_row = local_sums[0] + matches * incoming
    owned_rows = jnp.stack([head_row, local_sums[1]])
    owned_ids = (first_doc + jnp.arange(2, dtype=jnp.int32)).astype(jnp.float32)
    gathered, gathered_ids = (
        lax.all_gather(owned_rows, "ctx", axis=0, tiled=True),
        lax.all_gather(owned_ids, "ctx", axis=0, tiled=True),
    )
    positions = jnp.arange(gathered.shape[0], dtype=jnp.int32)
    wanted = jnp.arange(doc_count, dtype=jnp.int32).astype(jnp.float32)
    found = gathered_ids[None, :] == wanted[:, None]
    chosen = jnp.max(jnp.where(found, positions[None, :], -1), axis=1)
    doc_grads = jnp.take(gathered, chosen, axis=0)
    partial_q = jnp.dot(
        doc_grads, inverse, precision=lax.Precision.HIGHEST, preferred_element_type=jnp.float32
    )
    precond = lax.psum(partial_q, "col").astype(jnp.bfloat16)
    return lax.dot_general(
        lax.all_gather(precond, "ctx", axis=1, tiled=True),
        store_rows,
        (((1,), (1,)), ((), ())),
        preferred_element_type=jnp.float32,
    )


LANES = 128
ROWS = 8
SLOTS = 3
STEPS = 32767.0
LEAST = 2.0**-110
LEFT_CHUNKS = 1
RIGHT_CHUNKS = 4
MESH = pl.DeviceIdType.MESH
NT = (((1,), (1,)), ((), ()))


def halves(value):
    high = value.astype(jnp.bfloat16).astype(jnp.float32)
    return high, value - high


def dot_nt(left, right):
    return lax.dot_general(left, right, NT, preferred_element_type=jnp.float32)


def dot(left, right):
    return jnp.dot(left, right, preferred_element_type=jnp.float32)


def await_bytes(ref, sem):
    pltpu.make_async_copy(ref, ref, sem).wait()


def score_kernel(
    n, cols, docs,
    act, grad, ids, pin, pout, inv, store, out,
    xl, xr, inv_v, store_v, inv_hi, inv_lo, store_t, ids_v,
    part, came, full_l, codes, notes, tally, sums, q_part, q_from, q_all,
    load_sem, send_sem, recv_sem, ready,
):
    me = lax.axis_index("ctx")
    core = lax.axis_index("col")
    other = cols - 1 - core
    tokens = act.shape[0] * ROWS
    rank = pin.shape[0] * ROWS
    half = rank // cols
    pack = LANES // rank
    groups = half // pack
    piece = SLOTS * groups
    width = q_part.shape[1]
    spans = width // LANES

    barrier = pltpu.get_barrier_semaphore()
    ctx_peers = [{"ctx": there} for there in far_first(me, n)]
    peers = [peer | {"col": to} for peer in ctx_peers for to in (0, 1)]
    partner = {"col": other}

    @pl.when(core == cols - 1)
    def _():
        pl.semaphore_signal(barrier, inc=1, device_id=partner, device_id_type=MESH)

    for peer in ctx_peers:
        pl.semaphore_signal(barrier, inc=1, device_id=peer | {"col": cols - 1}, device_id_type=MESH)

    def load(src, dst, sem):
        pltpu.make_async_copy(src, dst, load_sem.at[sem]).start()

    stages = []
    for x, w, v, count in ((act, pin, xl, LEFT_CHUNKS), (grad, pout, xr, RIGHT_CHUNKS)):
        step = x.shape[1] // count
        for i in range(count):
            span = pl.ds(i * step, step)
            for source, row in ((x, 0), (w, tokens)):
                for j in range(source.shape[0]):
                    load(source.at[j, span], v.at[span, pl.ds(row + j * ROWS, ROWS)], len(stages))
            stages.append(v.at[span])
    ids_sem, inv_sem, store_sem = (len(stages) + i for i in range(3))
    load(ids, ids_v, ids_sem)
    load(inv, inv_v, inv_sem)
    load(store, store_v, store_sem)

    @pl.when(core == 0)
    def _():
        pl.semaphore_wait(barrier, 1)
        pl.semaphore_signal(ready, inc=1, device_id=partner, device_id_type=MESH)

    def send(src, dst, at, peer):
        pltpu.make_async_remote_copy(
            src_ref=src, dst_ref=dst, send_sem=send_sem.at[0], recv_sem=recv_sem.at[at],
            device_id=peer, device_id_type=MESH,
        ).start()

    totals = []
    for first, count in ((0, LEFT_CHUNKS), (LEFT_CHUNKS, RIGHT_CHUNKS)):
        total = None
        for i in range(first, first + count):
            await_bytes(stages[i], load_sem.at[i])
            tiles = stages[i].shape[0]
            cuts = 2 if i >= LEFT_CHUNKS + RIGHT_CHUNKS - 2 else 1
            terms = []
            for c in range(cuts):
                deep = jnp.concatenate(
                    [stages[i][k] for k in range(c * tiles // cuts, (c + 1) * tiles // cuts)], axis=1
                )
                terms.append(dot_nt(deep[tokens:], deep[:tokens]))
            term = sum(terms[1:], terms[0])
            total = term if total is None else total + term
        totals.append(total)
    left, right = totals
    part[:half] = left[:half]
    part[half : half + rank] = right
    part[half + rank :] = left[half:]
    @pl.when(core == cols - 1)
    def _():
        pl.semaphore_wait(ready, 1)

    span = pl.ds(pl.multiple_of(other * half, half), half + rank)
    send(part.at[span], came.at[span], 0, partner)

    @pl.when(core == cols - 1)
    def _():
        pl.semaphore_wait(barrier, cols * (n - 1))
        pl.semaphore_signal(ready, inc=1, device_id=partner, device_id_type=MESH)

    await_bytes(ids_v, load_sem.at[ids_sem])
    own_ids = ids_v[...]
    first = own_ids[:, 0:1]
    masks = [(own_ids == first + s).astype(jnp.float32) for s in range(SLOTS)]
    await_bytes(part.at[pl.ds(0, half + rank)], recv_sem.at[0])
    rows = pl.ds(pl.multiple_of(core * (half + rank), half), half)
    full_l[...] = part[rows, :] + came[rows, :]
    highs, lows = [], []
    for p in range(pack):
        lines = full_l[pl.ds(p, groups, stride=pack), :]
        high, low = halves(jnp.concatenate([lines * mask for mask in masks], axis=0))
        highs.append(high)
        lows.append(low)
    weights = jnp.concatenate(highs + highs + lows, axis=1).astype(jnp.bfloat16)
    high, low = halves(part[half : half + rank] + came[half : half + rank])
    zero = jnp.zeros_like(high)

    def diagonal(block, p):
        return [block if q == p else zero for q in range(pack)]

    spread = jnp.concatenate(
        [
            jnp.concatenate(diagonal(high, p) + diagonal(low, p) + diagonal(high, p), axis=1)
            for p in range(pack)
        ],
        axis=0,
    ).astype(jnp.bfloat16)
    mine = pl.ds(pl.multiple_of(me * piece, 2 * ROWS), piece)
    product = dot_nt(weights, spread)
    lane = lax.broadcasted_iota(jnp.int32, (1, LANES), 1)
    note = jnp.broadcast_to(first.astype(jnp.float32), (1, LANES))
    coded = []
    for s in range(SLOTS):
        rows_s = product[s * groups : (s + 1) * groups]
        top = jnp.max(jnp.max(jnp.abs(rows_s), axis=0, keepdims=True), axis=1, keepdims=True)
        top = jnp.maximum(top, LEAST)
        coded.append(jnp.floor(rows_s * (STEPS / top) + 0.5))
        note = jnp.where(lane > s, top * (1.0 / STEPS), note)
    notes[me] = note
    codes[mine, :] = jnp.concatenate(coded, axis=0).astype(jnp.int32).astype(jnp.int16)

    @pl.when(core == 0)
    def _():
        pl.semaphore_wait(ready, 1)

    for peer in ctx_peers:
        wave = 1 + 3 * (jnp.bitwise_xor(me, peer["ctx"]) // 2 % 2)
        send(notes.at[me], notes.at[me], wave, peer)
        send(codes.at[mine], codes.at[mine], wave, peer)

    await_bytes(inv_v, load_sem.at[inv_sem])
    band = LANES

    def split(i, carry):
        rows = pl.ds(pl.multiple_of(i * band, band), band)
        high, low = halves(inv_v[rows, :])
        inv_hi[rows, :] = high.astype(jnp.bfloat16)
        inv_lo[rows, :] = low.astype(jnp.bfloat16)
        return carry

    lax.fori_loop(0, inv_v.shape[0] // band, split, 0)
    await_bytes(store_v, load_sem.at[store_sem])
    stored = store_v.shape[0]
    for i in range(n * cols):
        tiles = []
        for j in range(spans):
            tile = (i * spans + j) * LANES
            tiles.append(store_v[:, tile : tile + LANES])
        store_t[i * LANES : (i + 1) * LANES, :] = jnp.concatenate(tiles, axis=0).T

    def decode(r):
        there = jnp.bitwise_xor(me, r)
        note = notes[there]
        block = codes[pl.ds(pl.multiple_of(there * piece, 2 * ROWS), piece), :].astype(jnp.int32).astype(jnp.float32)
        for s in range(SLOTS):
            rows = block[s * groups : (s + 1) * groups] * note[:, s + 1 : s + 2]
            sums[pl.ds(r * SLOTS + s, groups, stride=SLOTS * n), :] = rows

    decode(0)
    for wave, senders in ((4, n // 2), (1, n // 2 - 1)):
        await_bytes(tally.at[pl.ds(0, senders * (1 + piece // 2))], recv_sem.at[wave])
        for r in range(1, n):
            if (r // 2 % 2 == 1) == (wave == 4):
                decode(r)
    gathered = jnp.concatenate(
        [sums[k * SLOTS * n : (k + 1) * SLOTS * n, :] for k in range(groups)], axis=1
    )
    high, low = halves(gathered)
    both = jnp.concatenate([high, low], axis=0).astype(jnp.bfloat16)
    high = high.astype(jnp.bfloat16)
    doc_rows = q_part.shape[0]
    column = lax.broadcasted_iota(jnp.int32, (1, SLOTS * n), 1)
    doc_of = jnp.zeros((1, SLOTS * n), jnp.float32)
    for r in range(n):
        for s in range(SLOTS):
            doc_of = jnp.where(column == r * SLOTS + s, notes[jnp.bitwise_xor(me, r)][:, :1] + s, doc_of)
    docs_at = lax.broadcasted_iota(jnp.int32, (doc_rows, SLOTS * n), 0).astype(jnp.float32)
    pick = (docs_at == doc_of).astype(jnp.bfloat16)
    pick = jnp.concatenate([pick, pick, pick], axis=1)

    def picked(side):
        at = pl.ds(pl.multiple_of(side * width, width), width)
        main = dot(both, inv_hi[:, at])
        rows = main[: SLOTS * n] + main[SLOTS * n :] + dot(high, inv_lo[:, at])
        high_rows, rest = halves(rows)
        middle, low_rows = halves(rest)
        return dot(pick, jnp.concatenate([high_rows, middle, low_rows], axis=0).astype(jnp.bfloat16))

    q_part[...] = picked(other)
    send(q_part, q_from, 2, partner)
    own = picked(core)
    await_bytes(q_part, recv_sem.at[2])
    slot = me * cols + core
    total = own + q_from[...]
    q_all[slot] = jnp.concatenate(
        [total[:docs, j * LANES : (j + 1) * LANES] for j in range(spans)], axis=0
    ).astype(jnp.bfloat16)
    for peer in peers + [partner]:
        send(q_all.at[slot], q_all.at[slot], 3, peer)
    await_bytes(q_all.at[pl.ds(0, n * cols - 1)], recv_sem.at[3])
    precond = jnp.concatenate([q_all[i] for i in range(n * cols)], axis=1)
    scores = dot(precond, store_t[...])
    out[...] = sum(scores[j * docs : (j + 1) * docs, j * stored : (j + 1) * stored] for j in range(spans))
    await_bytes(tally, send_sem.at[0])


def far_first(me, n):
    rows = n // 2
    row, side = me // 2, me % 2
    upper = row >= rows // 2
    near = jnp.where(upper, rows - 1 - row, row)
    order = []
    for j in range(rows - 1):
        there = rows - 1 - j
        there = there - (there <= near).astype(jnp.int32)
        there = jnp.where(upper, rows - 1 - there, there)
        order += [2 * there + 1 - side, 2 * there + side]
    return order[:2] + [2 * row + 1 - side] + order[2:]


def tiled(x):
    rows, columns = x.shape
    return x.reshape(rows // ROWS, ROWS, columns // LANES, LANES).transpose(0, 2, 1, 3)


def fused(n, cols, activations, gradients, doc_ids, proj_in, proj_out, inverse, store_rows):
    tokens = activations.shape[0]
    rank = proj_in.shape[1]
    half = rank // cols
    docs = SLOTS * n // 2
    doc_rows = -(-docs // 16) * 16
    width = inverse.shape[1] // cols
    spans = width // LANES
    piece = SLOTS * half * rank // LANES
    sent = 4 * (half + rank) * tokens + (n - 1) * (4 + 2 * piece) * LANES + 4 * doc_rows * width
    sent += (n * cols - 1) * 2 * spans * docs * LANES
    anywhere = pl.BlockSpec(memory_space=pl.ANY)
    dma = pltpu.SemaphoreType.DMA
    return pl.pallas_call(
        functools.partial(score_kernel, n, cols, docs),
        name="scores",
        out_shape=pltpu.VMEM((docs, store_rows.shape[0]), jnp.float32),
        in_specs=[anywhere] * 7,
        out_specs=pl.BlockSpec(memory_space=pltpu.VMEM),
        scratch_shapes=[
            pltpu.VMEM((activations.shape[1] // LANES, tokens + rank, LANES), jnp.bfloat16),
            pltpu.VMEM((gradients.shape[1] // LANES, tokens + rank, LANES), jnp.bfloat16),
            pltpu.VMEM(inverse.shape, jnp.float32),
            pltpu.VMEM(store_rows.shape, jnp.bfloat16),
            pltpu.VMEM(inverse.shape, jnp.bfloat16),
            pltpu.VMEM(inverse.shape, jnp.bfloat16),
            pltpu.VMEM((store_rows.shape[1] // spans, spans * store_rows.shape[0]), jnp.bfloat16),
            pltpu.VMEM((1, tokens), jnp.int32),
            pltpu.VMEM((2 * half + rank, tokens), jnp.float32),
            pltpu.VMEM((2 * half + rank, tokens), jnp.float32),
            pltpu.VMEM((half, tokens), jnp.float32),
            pltpu.VMEM((n * piece, LANES), jnp.int16),
            pltpu.VMEM((n, 1, LANES), jnp.float32),
            pltpu.VMEM((sent // (4 * LANES), 1, LANES), jnp.float32),
            pltpu.VMEM((n * piece, LANES), jnp.float32),
            pltpu.VMEM((doc_rows, width), jnp.float32),
            pltpu.VMEM((doc_rows, width), jnp.float32),
            pltpu.VMEM((n * cols, spans * docs, LANES), jnp.bfloat16),
            dma((LEFT_CHUNKS + RIGHT_CHUNKS + 3,)),
            dma((1,)),
            dma((5,)),
            pltpu.SemaphoreType.REGULAR,
        ],
        compiler_params=pltpu.CompilerParams(
            collective_id=0, has_side_effects=True, vmem_limit_bytes=60 << 20
        ),
    )(tiled(activations), tiled(gradients), doc_ids[None, :], tiled(proj_in.T), tiled(proj_out.T), inverse, store_rows)


def suits_kernel(n, cols, activations, gradients, proj_in, inverse):
    rank = proj_in.shape[1]
    return (
        cols == 2
        and activations.shape[0] == LANES
        and LANES % rank == 0
        and (rank // cols * rank) % (ROWS * LANES) == 0
        and activations.shape[1] % (LEFT_CHUNKS * LANES) == 0
        and gradients.shape[1] % (RIGHT_CHUNKS * LANES) == 0
        and inverse.shape[1] % (cols * LANES) == 0
        and 8 <= n <= 16
        and n & (n - 1) == 0
    )


def solution(mesh):
    in_specs = (
        P(("groups", "ctx"), "col"),
        P(("groups", "ctx"), "col"),
        P(("groups", "ctx")),
        P("col", None),
        P("col", None),
        P("col", "ctx"),
        P(("groups", "ctx", "col"), None),
    )
    out_specs = P(None, ("groups", "ctx", "col"))
    n, cols = mesh.shape["ctx"], mesh.shape["col"]

    def body(activations, gradients, doc_ids, proj_in, proj_out, inverse, store_rows):
        args = (activations, gradients, doc_ids, proj_in, proj_out, inverse, store_rows)
        if suits_kernel(n, cols, activations, gradients, proj_in, inverse):
            return fused(n, cols, *args)
        return shards(*args)

    return jax.shard_map(body, mesh=mesh, in_specs=in_specs, out_specs=out_specs, check_vma=False)
```

```python
import functools

import jax
import jax.numpy as jnp
from jax import lax
from jax.experimental import pallas as pl
from jax.experimental.pallas import tpu as pltpu
from jax.sharding import PartitionSpec as P


def from_behind(block, axis, distance):
    devices = range(lax.axis_size(axis))
    route = [(i - distance, i) for i in devices if i - distance in devices]
    return lax.ppermute(block, axis, route)


def shards(activations, gradients, doc_ids, proj_in, proj_out, inverse, store_rows):
    left_part = jnp.dot(activations, proj_in, preferred_element_type=jnp.float32)
    right_part = jnp.dot(gradients, proj_out, preferred_element_type=jnp.float32)
    proj_left, proj_right = lax.psum((left_part, right_part), "col")
    proj_rank = proj_right.shape[1]
    half_rank = proj_rank // lax.axis_size("col")
    own_half = lax.dynamic_slice_in_dim(proj_left, lax.axis_index("col") * half_rank, half_rank, 1)
    first_doc = doc_ids[0]
    slot_index = doc_ids - first_doc
    onehot = (slot_index[:, None] == jnp.arange(3, dtype=jnp.int32)[None, :]).astype(jnp.float32)
    weighted = (onehot[:, :, None] * own_half[:, None, :]).reshape(own_half.shape[0], 3 * half_rank)
    local_sums = lax.dot_general(
        weighted,
        proj_right,
        (((0,), (0,)), ((), ())),
        precision=lax.Precision.HIGHEST,
        preferred_element_type=jnp.float32,
    ).reshape(3, half_rank * proj_rank)
    doc_count = 3 * lax.axis_size("ctx") // 2
    last_row = lax.dynamic_index_in_dim(local_sums, slot_index[-1], 0, keepdims=False)
    incoming, incoming_id = from_behind((last_row, doc_ids[-1].astype(jnp.float32)), "ctx", 1)
    matches = (incoming_id == first_doc.astype(jnp.float32)).astype(jnp.float32)
    head_row = local_sums[0] + matches * incoming
    owned_rows = jnp.stack([head_row, local_sums[1]])
    owned_ids = (first_doc + jnp.arange(2, dtype=jnp.int32)).astype(jnp.float32)
    gathered, gathered_ids = (
        lax.all_gather(owned_rows, "ctx", axis=0, tiled=True),
        lax.all_gather(owned_ids, "ctx", axis=0, tiled=True),
    )
    positions = jnp.arange(gathered.shape[0], dtype=jnp.int32)
    wanted = jnp.arange(doc_count, dtype=jnp.int32).astype(jnp.float32)
    found = gathered_ids[None, :] == wanted[:, None]
    chosen = jnp.max(jnp.where(found, positions[None, :], -1), axis=1)
    doc_grads = jnp.take(gathered, chosen, axis=0)
    partial_q = jnp.dot(
        doc_grads, inverse, precision=lax.Precision.HIGHEST, preferred_element_type=jnp.float32
    )
    precond = lax.psum(partial_q, "col").astype(jnp.bfloat16)
    return lax.dot_general(
        lax.all_gather(precond, "ctx", axis=1, tiled=True),
        store_rows,
        (((1,), (1,)), ((), ())),
        preferred_element_type=jnp.float32,
    )


LANES = 128
ROWS = 8
SLOTS = 3
STEPS = 32767.0
LEAST = 2.0**-110
LEFT_CHUNKS = 1
RIGHT_CHUNKS = 4
MESH = pl.DeviceIdType.MESH
NT = (((1,), (1,)), ((), ()))


def halves(value):
    high = value.astype(jnp.bfloat16).astype(jnp.float32)
    return high, value - high


def dot_nt(left, right):
    return lax.dot_general(left, right, NT, preferred_element_type=jnp.float32)


def dot(left, right):
    return jnp.dot(left, right, preferred_element_type=jnp.float32)


def await_bytes(ref, sem):
    pltpu.make_async_copy(ref, ref, sem).wait()


def score_kernel(
    n, cols, docs,
    act, grad, ids, pin, pout, inv, store, out,
    xl, xr, inv_v, store_v, inv_hi, inv_lo, store_t, ids_v,
    part, came, full_l, codes, notes, tally, sums, q_part, q_from, q_all,
    load_sem, send_sem, recv_sem, ready,
):
    me = lax.axis_index("ctx")
    core = lax.axis_index("col")
    other = cols - 1 - core
    tokens = act.shape[0] * ROWS
    rank = pin.shape[0] * ROWS
    half = rank // cols
    pack = LANES // rank
    groups = half // pack
    piece = SLOTS * groups
    width = q_part.shape[1]
    spans = width // LANES

    barrier = pltpu.get_barrier_semaphore()
    ctx_peers = [{"ctx": there} for there in far_first(me, n)]
    peers = [peer | {"col": to} for peer in ctx_peers for to in (0, 1)]
    partner = {"col": other}

    @pl.when(core == cols - 1)
    def _():
        pl.semaphore_signal(barrier, inc=1, device_id=partner, device_id_type=MESH)

    for peer in ctx_peers:
        pl.semaphore_signal(barrier, inc=1, device_id=peer | {"col": cols - 1}, device_id_type=MESH)

    def load(src, dst, sem):
        pltpu.make_async_copy(src, dst, load_sem.at[sem]).start()

    stages = []
    for x, w, v, count in ((act, pin, xl, LEFT_CHUNKS), (grad, pout, xr, RIGHT_CHUNKS)):
        step = x.shape[1] // count
        for i in range(count):
            span = pl.ds(i * step, step)
            for source, row in ((x, 0), (w, tokens)):
                for j in range(source.shape[0]):
                    load(source.at[j, span], v.at[span, pl.ds(row + j * ROWS, ROWS)], len(stages))
            stages.append(v.at[span])
    ids_sem, inv_sem, store_sem = (len(stages) + i for i in range(3))
    load(ids, ids_v, ids_sem)
    load(inv, inv_v, inv_sem)
    load(store, store_v, store_sem)

    @pl.when(core == 0)
    def _():
        pl.semaphore_wait(barrier, 1)
        pl.semaphore_signal(ready, inc=1, device_id=partner, device_id_type=MESH)

    def send(src, dst, at, peer):
        pltpu.make_async_remote_copy(
            src_ref=src, dst_ref=dst, send_sem=send_sem.at[0], recv_sem=recv_sem.at[at],
            device_id=peer, device_id_type=MESH,
        ).start()

    totals = []
    for first, count in ((0, LEFT_CHUNKS), (LEFT_CHUNKS, RIGHT_CHUNKS)):
        total = None
        for i in range(first, first + count):
            await_bytes(stages[i], load_sem.at[i])
            deep = jnp.concatenate([stages[i][k] for k in range(stages[i].shape[0])], axis=1)
            term = dot_nt(deep[tokens:], deep[:tokens])
            total = term if total is None else total + term
        totals.append(total)
    left, right = totals
    part[:half] = left[:half]
    part[half : half + rank] = right
    part[half + rank :] = left[half:]
    @pl.when(core == cols - 1)
    def _():
        pl.semaphore_wait(ready, 1)

    span = pl.ds(pl.multiple_of(other * half, half), half + rank)
    send(part.at[span], came.at[span], 0, partner)

    @pl.when(core == cols - 1)
    def _():
        pl.semaphore_wait(barrier, cols * (n - 1))
        pl.semaphore_signal(ready, inc=1, device_id=partner, device_id_type=MESH)

    await_bytes(ids_v, load_sem.at[ids_sem])
    own_ids = ids_v[...]
    first = own_ids[:, 0:1]
    masks = [(own_ids == first + s).astype(jnp.float32) for s in range(SLOTS)]
    await_bytes(part.at[pl.ds(0, half + rank)], recv_sem.at[0])
    rows = pl.ds(pl.multiple_of(core * (half + rank), half), half)
    full_l[...] = part[rows, :] + came[rows, :]
    highs, lows = [], []
    for p in range(pack):
        lines = full_l[pl.ds(p, groups, stride=pack), :]
        high, low = halves(jnp.concatenate([lines * mask for mask in masks], axis=0))
        highs.append(high)
        lows.append(low)
    weights = jnp.concatenate(highs + highs + lows, axis=1).astype(jnp.bfloat16)
    high, low = halves(part[half : half + rank] + came[half : half + rank])
    zero = jnp.zeros_like(high)

    def diagonal(block, p):
        return [block if q == p else zero for q in range(pack)]

    spread = jnp.concatenate(
        [
            jnp.concatenate(diagonal(high, p) + diagonal(low, p) + diagonal(high, p), axis=1)
            for p in range(pack)
        ],
        axis=0,
    ).astype(jnp.bfloat16)
    mine = pl.ds(pl.multiple_of(me * piece, 2 * ROWS), piece)
    product = dot_nt(weights, spread)
    lane = lax.broadcasted_iota(jnp.int32, (1, LANES), 1)
    note = jnp.broadcast_to(first.astype(jnp.float32), (1, LANES))
    coded = []
    for s in range(SLOTS):
        rows_s = product[s * groups : (s + 1) * groups]
        top = jnp.max(jnp.max(jnp.abs(rows_s), axis=0, keepdims=True), axis=1, keepdims=True)
        top = jnp.maximum(top, LEAST)
        coded.append(jnp.floor(rows_s * (STEPS / top) + 0.5))
        note = jnp.where(lane > s, top * (1.0 / STEPS), note)
    notes[me] = note
    codes[mine, :] = jnp.concatenate(coded, axis=0).astype(jnp.int32).astype(jnp.int16)

    @pl.when(core == 0)
    def _():
        pl.semaphore_wait(ready, 1)

    for peer in ctx_peers:
        wave = 1 + 3 * (jnp.bitwise_xor(me, peer["ctx"]) // 2 % 2)
        send(notes.at[me], notes.at[me], wave, peer)
        send(codes.at[mine], codes.at[mine], wave, peer)

    await_bytes(inv_v, load_sem.at[inv_sem])
    band = LANES

    def split(i, carry):
        rows = pl.ds(pl.multiple_of(i * band, band), band)
        high, low = halves(inv_v[rows, :])
        inv_hi[rows, :] = high.astype(jnp.bfloat16)
        inv_lo[rows, :] = low.astype(jnp.bfloat16)
        return carry

    lax.fori_loop(0, inv_v.shape[0] // band, split, 0)
    await_bytes(store_v, load_sem.at[store_sem])
    stored = store_v.shape[0]
    for i in range(n * cols):
        tiles = []
        for j in range(spans):
            tile = (i * spans + j) * LANES
            tiles.append(store_v[:, tile : tile + LANES])
        store_t[i * LANES : (i + 1) * LANES, :] = jnp.concatenate(tiles, axis=0).T

    def decode(r):
        there = jnp.bitwise_xor(me, r)
        note = notes[there]
        block = codes[pl.ds(pl.multiple_of(there * piece, 2 * ROWS), piece), :].astype(jnp.int32).astype(jnp.float32)
        for s in range(SLOTS):
            rows = block[s * groups : (s + 1) * groups] * note[:, s + 1 : s + 2]
            sums[pl.ds(r * SLOTS + s, groups, stride=SLOTS * n), :] = rows

    decode(0)
    for wave, senders in ((4, n // 2), (1, n // 2 - 1)):
        await_bytes(tally.at[pl.ds(0, senders * (1 + piece // 2))], recv_sem.at[wave])
        for r in range(1, n):
            if (r // 2 % 2 == 1) == (wave == 4):
                decode(r)
    gathered = jnp.concatenate(
        [sums[k * SLOTS * n : (k + 1) * SLOTS * n, :] for k in range(groups)], axis=1
    )
    high, low = halves(gathered)
    both = jnp.concatenate([high, low], axis=0).astype(jnp.bfloat16)
    high = high.astype(jnp.bfloat16)
    doc_rows = q_part.shape[0]
    column = lax.broadcasted_iota(jnp.int32, (1, SLOTS * n), 1)
    doc_of = jnp.zeros((1, SLOTS * n), jnp.float32)
    for r in range(n):
        for s in range(SLOTS):
            doc_of = jnp.where(column == r * SLOTS + s, notes[jnp.bitwise_xor(me, r)][:, :1] + s, doc_of)
    docs_at = lax.broadcasted_iota(jnp.int32, (doc_rows, SLOTS * n), 0).astype(jnp.float32)
    pick = (docs_at == doc_of).astype(jnp.bfloat16)
    pick = jnp.concatenate([pick, pick, pick], axis=1)

    def picked(side):
        at = pl.ds(pl.multiple_of(side * width, width), width)
        main = dot(both, inv_hi[:, at])
        rows = main[: SLOTS * n] + main[SLOTS * n :] + dot(high, inv_lo[:, at])
        high_rows, rest = halves(rows)
        middle, low_rows = halves(rest)
        return dot(pick, jnp.concatenate([high_rows, middle, low_rows], axis=0).astype(jnp.bfloat16))

    q_part[...] = picked(other)
    send(q_part, q_from, 2, partner)
    own = picked(core)
    await_bytes(q_part, recv_sem.at[2])
    slot = me * cols + core
    total = own + q_from[...]
    q_all[slot] = jnp.concatenate(
        [total[:docs, j * LANES : (j + 1) * LANES] for j in range(spans)], axis=0
    ).astype(jnp.bfloat16)
    for peer in peers + [partner]:
        send(q_all.at[slot], q_all.at[slot], 3, peer)
    await_bytes(q_all.at[pl.ds(0, n * cols - 1)], recv_sem.at[3])
    precond = jnp.concatenate([q_all[i] for i in range(n * cols)], axis=1)
    scores = dot(precond, store_t[...])
    out[...] = sum(scores[j * docs : (j + 1) * docs, j * stored : (j + 1) * stored] for j in range(spans))
    await_bytes(tally, send_sem.at[0])


def far_first(me, n):
    rows = n // 2
    row, side = me // 2, me % 2
    upper = row >= rows // 2
    near = jnp.where(upper, rows - 1 - row, row)
    order = []
    for j in range(rows - 1):
        there = rows - 1 - j
        there = there - (there <= near).astype(jnp.int32)
        there = jnp.where(upper, rows - 1 - there, there)
        order += [2 * there + 1 - side, 2 * there + side]
    return order[:2] + [2 * row + 1 - side] + order[2:]


def tiled(x):
    rows, columns = x.shape
    return x.reshape(rows // ROWS, ROWS, columns // LANES, LANES).transpose(0, 2, 1, 3)


def fused(n, cols, activations, gradients, doc_ids, proj_in, proj_out, inverse, store_rows):
    tokens = activations.shape[0]
    rank = proj_in.shape[1]
    half = rank // cols
    docs = SLOTS * n // 2
    doc_rows = -(-docs // 16) * 16
    width = inverse.shape[1] // cols
    spans = width // LANES
    piece = SLOTS * half * rank // LANES
    sent = 4 * (half + rank) * tokens + (n - 1) * (4 + 2 * piece) * LANES + 4 * doc_rows * width
    sent += (n * cols - 1) * 2 * spans * docs * LANES
    anywhere = pl.BlockSpec(memory_space=pl.ANY)
    dma = pltpu.SemaphoreType.DMA
    return pl.pallas_call(
        functools.partial(score_kernel, n, cols, docs),
        name="scores",
        out_shape=pltpu.VMEM((docs, store_rows.shape[0]), jnp.float32),
        in_specs=[anywhere] * 7,
        out_specs=pl.BlockSpec(memory_space=pltpu.VMEM),
        scratch_shapes=[
            pltpu.VMEM((activations.shape[1] // LANES, tokens + rank, LANES), jnp.bfloat16),
            pltpu.VMEM((gradients.shape[1] // LANES, tokens + rank, LANES), jnp.bfloat16),
            pltpu.VMEM(inverse.shape, jnp.float32),
            pltpu.VMEM(store_rows.shape, jnp.bfloat16),
            pltpu.VMEM(inverse.shape, jnp.bfloat16),
            pltpu.VMEM(inverse.shape, jnp.bfloat16),
            pltpu.VMEM((store_rows.shape[1] // spans, spans * store_rows.shape[0]), jnp.bfloat16),
            pltpu.VMEM((1, tokens), jnp.int32),
            pltpu.VMEM((2 * half + rank, tokens), jnp.float32),
            pltpu.VMEM((2 * half + rank, tokens), jnp.float32),
            pltpu.VMEM((half, tokens), jnp.float32),
            pltpu.VMEM((n * piece, LANES), jnp.int16),
            pltpu.VMEM((n, 1, LANES), jnp.float32),
            pltpu.VMEM((sent // (4 * LANES), 1, LANES), jnp.float32),
            pltpu.VMEM((n * piece, LANES), jnp.float32),
            pltpu.VMEM((doc_rows, width), jnp.float32),
            pltpu.VMEM((doc_rows, width), jnp.float32),
            pltpu.VMEM((n * cols, spans * docs, LANES), jnp.bfloat16),
            dma((LEFT_CHUNKS + RIGHT_CHUNKS + 3,)),
            dma((1,)),
            dma((5,)),
            pltpu.SemaphoreType.REGULAR,
        ],
        compiler_params=pltpu.CompilerParams(
            collective_id=0, has_side_effects=True, vmem_limit_bytes=60 << 20
        ),
    )(tiled(activations), tiled(gradients), doc_ids[None, :], tiled(proj_in.T), tiled(proj_out.T), inverse, store_rows)


def suits_kernel(n, cols, activations, gradients, proj_in, inverse):
    rank = proj_in.shape[1]
    return (
        cols == 2
        and activations.shape[0] == LANES
        and LANES % rank == 0
        and (rank // cols * rank) % (ROWS * LANES) == 0
        and activations.shape[1] % (LEFT_CHUNKS * LANES) == 0
        and gradients.shape[1] % (RIGHT_CHUNKS * LANES) == 0
        and inverse.shape[1] % (cols * LANES) == 0
        and 8 <= n <= 16
        and n & (n - 1) == 0
    )


def solution(mesh):
    in_specs = (
        P(("groups", "ctx"), "col"),
        P(("groups", "ctx"), "col"),
        P(("groups", "ctx")),
        P("col", None),
        P("col", None),
        P("col", "ctx"),
        P(("groups", "ctx", "col"), None),
    )
    out_specs = P(None, ("groups", "ctx", "col"))
    n, cols = mesh.shape["ctx"], mesh.shape["col"]

    def body(activations, gradients, doc_ids, proj_in, proj_out, inverse, store_rows):
        args = (activations, gradients, doc_ids, proj_in, proj_out, inverse, store_rows)
        if suits_kernel(n, cols, activations, gradients, proj_in, inverse):
            return fused(n, cols, *args)
        return shards(*args)

    return jax.shard_map(body, mesh=mesh, in_specs=in_specs, out_specs=out_specs, check_vma=False)
```
